256 devices in a mesh: dev: 256 (over x, y, z, core).
Axes of the slice: x: 4, y: 4, z: 8, core: 2. Of those that a mesh axis runs over, the one named last changes fastest.
Arguments:
- field: float32 [16, 16, 16, 32768], P(None, None, None, 'dev'), may hold values from -6 to 6
- s_mats: float32 [3, 18, 18], replicated, may hold values from -1.5 to 1.5
- lam: float32 [3, 18], replicated, may hold values from 0.2 to 4
- coeff: float32 [3, 32768], P(None, 'dev'), may hold values from 0.5 to 2
- nbr_src: int32 [6, 32768], P(None, 'dev'), may hold values from 0 to 7, as said below
- nbr_idx: int32 [6, 32768], P(None, 'dev'), may hold values from 0 to 767, as said below
- orient: int32 [6, 32768], P(None, 'dev'), may hold values from 0 to 3, as said below
- send_x: int32 [2, 4096], P(None, 'dev'), may hold values from 0 to 255, as said below
- send_y: int32 [2, 4096], P(None, 'dev'), may hold values from 256 to 511, as said below
- send_z: int32 [2, 16384], P(None, 'dev'), may hold values from 512 to 767, as said below
Outputs:
- smoothed: float32 [16, 16, 16, 32768], P(None, None, None, 'dev')
The draws below stay inside these ranges and needn't reach their ends.
Inputs may be any that keep to these rules, and one draw needn't show every extreme that they name: `nbr_src`: 0 where the face lies on the boundary of the box of elements, 1 where the element across it is on the same device, 2 + j where it is on the device whose index is lower by o_j. Devices form a 4 x 4 x 16 grid, first index fastest; each holds a 8 x 8 x 2 block of the box, its elements in slots in any order and each stored mirrored or not along each of its three axes. Every face not on the boundary is shared by exactly two elements and listed from both sides. `nbr_idx`: for code 1 the id g * 128 + s of the face g of the element in slot s that meets this face; for code 2 + j a position in list j of the sending device; 0 for code 0. `orient`: the two sides of a shared face carry the same code; 0 on the boundary. `send_x`: row r (list r) holds the ids of the 16 faces of this device's block on its low (r = 0) or high (r = 1) side across the first dimension, each once, ordered by the faces' block coordinates along the second dimension, then the third; the device whose index is higher by o_r reads it. Each id is that of face 0 or 1 of its element. `send_y`: as send_x, across the second dimension (lists 2 and 3), 16 faces ordered by the first block coordinate, then the third; each id is that of face 2 or 3 of its element. `send_z`: as send_x, across the third dimension (lists 4 and 5), 64 faces ordered by the first block coordinate, then the second; each id is that of face 4 or 5 of its element.
All inputs are finite; a program needn't handle non-finite values.
Results may differ from the reference program's by a relative error of at most 0.0003.
Values sent between devices are 32-bit elements; how exact they have to be, the bound alone decides.
A program may use at most 128 MiB of HBM per device.

```python
import math
import jax
import jax.numpy as jnp
from jax import lax

NP = 16
NE = 18
BX = 8
BY = 8
BZ = 2
DEV_X = 4
DEV_Y = 4
ELEMS = 32768
N_DEV = 256


def block_tables(key):
    slots = BX * BY * BZ
    height = N_DEV // (DEV_X * DEV_Y)
    extents = (BX, BY, BZ)
    layout = (DEV_X, DEV_Y, height)
    device_step = (1, DEV_X, DEV_X * DEV_Y)
    place_step = (1, BX, BX * BY)
    keys = jax.random.split(jax.random.fold_in(key, 7), N_DEV)
    storage = jax.vmap(lambda part_key: jax.random.permutation(part_key, slots))(keys).astype(jnp.int32)
    placing = jnp.argsort(storage, axis=1).astype(jnp.int32)
    mirror = jax.random.randint(jax.random.fold_in(key, 8), (3, N_DEV, slots), 0, 2, dtype=jnp.int32)
    device = jnp.arange(N_DEV, dtype=jnp.int32)[:, None]
    local = (placing % BX, placing // BX % BY, placing // (BX * BY))
    owner = (device % DEV_X, device // DEV_X % DEV_Y, device // (DEV_X * DEV_Y))
    own_mirror = [jnp.take_along_axis(mirror[axis], placing, axis=1) for axis in range(3)]
    sources = []
    indices = []
    codes = []
    for face in range(6):
        axis = face // 2
        others = [other for other in range(3) if other != axis]
        side = face % 2 ^ own_mirror[axis]
        coord = owner[axis] * extents[axis] + local[axis]
        moved = coord + 2 * side - 1
        inside = (moved >= 0) & (moved < extents[axis] * layout[axis])
        moved = jnp.clip(moved, 0, extents[axis] * layout[axis] - 1)
        other_dev = device + (moved // extents[axis] - owner[axis]) * device_step[axis]
        other_place = placing + (moved % extents[axis] - local[axis]) * place_step[axis]
        flat_index = other_dev * slots + other_place
        other_slot = storage.reshape(-1)[flat_index]
        other_mirror = [mirror[other].reshape(-1)[flat_index] for other in range(3)]
        facing = 2 * axis + (1 - side ^ other_mirror[axis])
        code = (own_mirror[others[0]] ^ other_mirror[others[0]]) + 2 * (own_mirror[others[1]] ^ other_mirror[others[1]])
        same = other_dev == device
        position = local[others[0]] + extents[others[0]] * local[others[1]]
        sources.append(jnp.where(inside, jnp.where(same, 1, 2 + 2 * axis + 1 - side), 0))
        indices.append(jnp.where(inside, jnp.where(same, facing * slots + other_slot, position), 0))
        codes.append(jnp.where(inside, code, 0))
    sends = []
    for axis in range(3):
        others = [other for other in range(3) if other != axis]
        count = extents[others[0]] * extents[others[1]]
        position = jnp.arange(count, dtype=jnp.int32)
        rows = []
        for side in range(2):
            coords = [0, 0, 0]
            coords[axis] = (extents[axis] - 1) * side
            coords[others[0]] = position % extents[others[0]]
            coords[others[1]] = position // extents[others[0]]
            spot = coords[0] + BX * coords[1] + BX * BY * coords[2]
            slot = storage[:, spot]
            flip = mirror[axis][:, spot]
            face = 2 * axis + (side ^ flip)
            rows.append((face * slots + slot).reshape(-1))
        sends.append(jnp.stack(rows).astype(jnp.int32))
    shape = (6, N_DEV * slots)
    return (jnp.stack(sources).reshape(shape).astype(jnp.int32), jnp.stack(indices).reshape(shape).astype(jnp.int32), jnp.stack(codes).reshape(shape).astype(jnp.int32), sends[0], sends[1], sends[2])


def draw_nbr_src(key, part):
    return block_tables(key)[0]


def draw_nbr_idx(key, part):
    return block_tables(key)[1]


def draw_orient(key, part):
    return block_tables(key)[2]


def draw_send_x(key, part):
    return block_tables(key)[3]


def draw_send_y(key, part):
    return block_tables(key)[4]


def draw_send_z(key, part):
    return block_tables(key)[5]


def shard_levels(own_key, extent, cuts, least, top_value):
    loudness = 1.0
    for dim, parts in cuts:
        draws = jax.random.uniform(jax.random.fold_in(jax.random.fold_in(own_key, 6), dim), (parts,), jnp.float32, least / len(cuts), top_value / len(cuts))
        loudness = loudness * jnp.repeat(jnp.exp(draws), extent[dim] // parts).reshape((-1,) + (1,) * (len(extent) - 1 - dim))
    return loudness


def noise(stream_key, shape, scale, reach, shards=(), kind=jnp.bfloat16):
    drawn = jax.random.normal(stream_key, shape, jnp.float32) * scale
    if len(shards) > 0:
        drawn = shard_levels(stream_key, shape, shards, -0.22, 0.18) * drawn
    return jnp.clip(drawn, min=-reach, max=reach).astype(kind)


def setup_inputs(seed: int = 0) -> dict:
    seeds = jax.random.split(jax.random.key(seed), 11)
    return {
        "field": noise(seeds[0], (NP, NP, NP, ELEMS), 1.0, 6.0, ((3, 256),), jnp.float32),
        "s_mats": noise(seeds[1], (3, NE, NE), NE ** -0.5, 1.5, (), jnp.float32),
        "lam": jnp.clip(jnp.exp(jax.random.uniform(seeds[2], (3, NE), jnp.float32, math.log(0.2), math.log(4.0))), 0.2, 4.0),
        "coeff": jnp.clip(jnp.exp(math.log(2.0) - 1.3862944 * jax.random.uniform(seeds[3], (3, ELEMS), jnp.float32) ** shard_levels(seeds[3], (3, ELEMS), ((1, 256),), -0.2, 0.2)), 0.5, 2.0),
        "nbr_src": draw_nbr_src(jax.random.fold_in(seeds[10], 71), 0),
        "nbr_idx": draw_nbr_idx(jax.random.fold_in(seeds[10], 71), 0),
        "orient": draw_orient(jax.random.fold_in(seeds[10], 71), 0),
        "send_x": draw_send_x(jax.random.fold_in(seeds[10], 71), 0),
        "send_y": draw_send_y(jax.random.fold_in(seeds[10], 71), 0),
        "send_z": draw_send_z(jax.random.fold_in(seeds[10], 71), 0),
    }


EXACT = lax.Precision.HIGHEST


def face_planes(block):
    last = block.shape[0] - 2
    return jnp.concatenate([block[1], block[last], block[:, 1], block[:, last], block[:, :, 1], block[:, :, last]], axis=2)


def reorient(planes, codes):
    first = (codes % 2 == 1)[None, None]
    second = (codes // 2 == 1)[None, None]
    planes = jnp.where(first, jnp.flip(planes, 0), planes)
    return jnp.where(second, jnp.flip(planes, 1), planes)


def extend_box(block, ghosts):
    box = jnp.pad(block, ((1, 1), (1, 1), (1, 1), (0, 0)))
    last = box.shape[0] - 1
    box = box.at[0, 1:last, 1:last].set(ghosts[:, :, 0])
    box = box.at[last, 1:last, 1:last].set(ghosts[:, :, 1])
    box = box.at[1:last, 0, 1:last].set(ghosts[:, :, 2])
    box = box.at[1:last, last, 1:last].set(ghosts[:, :, 3])
    box = box.at[1:last, 1:last, 0].set(ghosts[:, :, 4])
    return box.at[1:last, 1:last, last].set(ghosts[:, :, 5])


def rim_layers(box):
    last = box.shape[0] - 1
    inner = slice(1, last)
    return jnp.stack([box[0, inner, inner], box[last, inner, inner], box[inner, 0, inner],
                      box[inner, last, inner], box[inner, inner, 0], box[inner, inner, last]], axis=2)


def add_layers(block, returned):
    last = block.shape[0] - 2
    block = block.at[1].add(returned[:, :, 0])
    block = block.at[last].add(returned[:, :, 1])
    block = block.at[:, 1].add(returned[:, :, 2])
    block = block.at[:, last].add(returned[:, :, 3])
    block = block.at[:, :, 1].add(returned[:, :, 4])
    return block.at[:, :, last].add(returned[:, :, 5])


def eigen_divisor(lam, scale):
    return (scale[0][None, None, None, :] * lam[0][:, None, None, None]
            + scale[1][None, None, None, :] * lam[1][None, :, None, None]
            + scale[2][None, None, None, :] * lam[2][None, None, :, None])


def solve_box(box, s_mats, divisor):
    coef = jnp.einsum('ia,ijkm->ajkm', s_mats[0], box, precision=EXACT)
    coef = jnp.einsum('jb,ajkm->abkm', s_mats[1], coef, precision=EXACT)
    coef = jnp.einsum('kc,abkm->abcm', s_mats[2], coef, precision=EXACT)
    scaled = coef / divisor
    solved = jnp.einsum('ia,abcm->ibcm', s_mats[0], scaled, precision=EXACT)
    solved = jnp.einsum('jb,ibcm->ijcm', s_mats[1], solved, precision=EXACT)
    return jnp.einsum('kc,ijcm->ijkm', s_mats[2], solved, precision=EXACT)


def reference(field, s_mats, lam, coeff, nbr_src, nbr_idx, orient, send_x, send_y, send_z):
    slots = BX * BY * BZ
    count = slots * N_DEV
    edge = field.shape[0]
    pool = jnp.concatenate([face_planes(field), jnp.zeros((edge, edge, 1), field.dtype)], axis=2)
    device = jnp.arange(count, dtype=jnp.int32) // slots
    offsets = (-1, 1, -DEV_X, DEV_X, -DEV_X * DEV_Y, DEV_X * DEV_Y)
    lists = (send_x[0], send_x[1], send_y[0], send_y[1], send_z[0], send_z[1])
    target = (nbr_idx // slots) * count + device * slots + nbr_idx % slots
    for direction in range(6):
        table = lists[direction]
        length = table.shape[0] // N_DEV
        sender = jnp.clip(device - offsets[direction], 0, N_DEV - 1)
        entry = table[jnp.clip(sender * length + nbr_idx, 0, table.shape[0] - 1)]
        remote = (entry // slots) * count + sender * slots + entry % slots
        target = jnp.where(nbr_src == 2 + direction, remote, target)
    target = jnp.where(nbr_src == 0, 6 * count, target).astype(jnp.int32)

    def one_device(number):
        start = number * slots
        block = lax.dynamic_slice_in_dim(field, start, slots, 3)
        where_from = lax.dynamic_slice_in_dim(target, start, slots, 1)
        codes = lax.dynamic_slice_in_dim(orient, start, slots, 1)
        scale = lax.dynamic_slice_in_dim(coeff, start, slots, 1)
        gathered = jnp.take(pool, where_from.reshape(-1), axis=2).reshape(edge, edge, 6, slots)
        ghosts = reorient(gathered, codes)
        solved = solve_box(extend_box(block, ghosts), s_mats, eigen_divisor(lam, scale))
        last = solved.shape[0] - 1
        return solved[1:last, 1:last, 1:last], reorient(rim_layers(solved), codes)

    inside, rims = lax.map(one_device, jnp.arange(N_DEV, dtype=jnp.int32))
    inside = jnp.moveaxis(inside, 0, 3).reshape(edge, edge, edge, count)
    values = jnp.transpose(rims, (1, 2, 3, 0, 4)).reshape(edge, edge, 6 * count)
    collected = jnp.zeros((edge, edge, 6 * count + 1), field.dtype).at[:, :, target.reshape(-1)].add(values)
    returned = collected[:, :, :6 * count].reshape(edge, edge, 6, count)
    return add_layers(inside, returned)
```

```python
import functools

import jax
import jax.numpy as jnp
import numpy as np
from jax import lax
from jax.experimental import pallas as pl
from jax.experimental.pallas import tpu as pltpu
from jax.sharding import PartitionSpec as P

NP = 16
NE = 18
SLOTS = 128
ROWS = 336
RIM = 320
COUNTS = (16, 16, 64)
STARTS = (0, 32, 64)
OFFSETS = (-1, 1, -4, 4, -16, 16)
BF = jnp.bfloat16
F32 = jnp.float32
VMEM = pl.BlockSpec(memory_space=pltpu.VMEM)


def make_tables():
    r = np.arange(ROWS)
    fits = r < NE * NE
    rb = np.zeros((ROWS, 96))
    rc = np.zeros((ROWS, 96))
    ra = np.zeros((NE * 8, 96))
    for t in range(3):
        rb[r[fits], t * 32 + r[fits] // NE] = 1
        rc[r[fits], t * 32 + r[fits] % NE] = 1
        ra[np.arange(NE * 8), t * 32 + np.arange(NE * 8) // 8] = 1
    inner = np.arange(1, 17)
    low, high = np.zeros(16, int), np.full(16, 17)
    jq = np.concatenate([np.repeat(inner, 16), low, high, inner, inner])
    kq = np.concatenate([np.tile(inner, 16), inner, inner, low, high])
    rj = np.zeros((RIM, 96))
    rk = np.zeros((RIM, 96))
    for t in range(3):
        rj[np.arange(RIM), t * 32 + jq] = 1
        rk[np.arange(RIM), t * 32 + kq] = 1
    cols = np.concatenate([np.arange(256), np.tile(np.arange(256, 320), 3)])
    qj = np.zeros((32, 512))
    qk = np.zeros((32, 512))
    qj[jq[cols], np.arange(448)] = 1
    qk[kq[cols], np.arange(448)] = 1
    qi = np.zeros((32, 512))
    c = np.arange(432)
    qi[(c % 144) // 8, c] = 1
    qb = np.zeros((32, 1024))
    qc = np.zeros((32, 1024))
    c = np.arange(1008)
    c = c[c % ROWS < NE * NE]
    qb[c % ROWS // NE, c] = 1
    qc[c % ROWS % NE, c] = 1
    flip = np.zeros((256, 256))
    n = np.arange(256)
    flip[n, n // 16 * 16 + 15 - n % 16] = 1
    left = np.concatenate([rb, rc, ra, rj, rk])
    right = np.concatenate([qj, qk, qi, qb[:, :512], qb[:, 512:], qc[:, :512], qc[:, 512:]])
    return left, right, flip


def split2(x):
    high = x.astype(BF)
    return high, (x - high.astype(F32)).astype(BF)


def split3(x):
    high = x.astype(BF)
    rest = x - high.astype(F32)
    middle = rest.astype(BF)
    return high, middle, (rest - middle.astype(F32)).astype(BF)


def dot(a, b):
    return jnp.dot(a, b, preferred_element_type=F32)


def widen(small, right):
    return sum(dot(term, right) for term in split3(small))


def deepen(left, small):
    return dot(left, jnp.concatenate(split3(small), axis=0))


def pick(condition):
    return jnp.where(condition, 1.0, 0.0).astype(BF)


def make_messages(planes, send, msgs):
    for axis in (2, 0, 1):
        count = 2 * COUNTS[axis]
        ids = send[axis : axis + 1, :] - 256 * axis
        chosen = pick(lax.broadcasted_iota(jnp.int32, (256, SLOTS), 0) == ids)
        high, low = split2(planes[axis])
        found = dot(high, chosen) + dot(low, chosen)
        msgs[STARTS[axis] : STARTS[axis] + count, :] = found.T[:count]


def list_rows(direction):
    axis, side = direction // 2, direction % 2
    return STARTS[axis] + side * COUNTS[axis], COUNTS[axis]


def greet(me):
    barrier = pltpu.get_barrier_semaphore()
    for offset in OFFSETS:
        pl.semaphore_signal(
            barrier, inc=1, device_id=(lax.rem(me + offset + 256, 256),), device_id_type=pl.DeviceIdType.MESH
        )
    pl.semaphore_wait(barrier, 6)


def start_copies(me, msgs, arrived, send_sem, recv_sem):
    copies = []
    for direction in (4, 5, 2, 3, 0, 1):
        start, count = list_rows(direction)
        copy = pltpu.make_async_remote_copy(
            src_ref=msgs.at[pl.ds(start, count)],
            dst_ref=arrived.at[pl.ds(start, count)],
            send_sem=send_sem.at[direction],
            recv_sem=recv_sem.at[direction],
            device_id=(lax.rem(me + OFFSETS[direction] + 256, 256),),
            device_id_type=pl.DeviceIdType.MESH,
        )
        copy.start()
        copies.append(copy)
    return copies


def reorient(planes, codes, flip):
    turned = jnp.concatenate([planes[16 * (15 - u) : 16 * (16 - u)] for u in range(16)], axis=0)
    planes = jnp.where(codes % 2 == 1, turned, planes)
    high, low = split2(planes)
    return jnp.where(codes >= 2, dot(flip, high) + dot(flip, low), planes)


def pair(table, axis):
    return jnp.concatenate([table[2 * axis : 2 * axis + 1, :], table[2 * axis + 1 : 2 * axis + 2, :]], axis=1)


def gather(axis, planes, arrived, nbr_src, nbr_idx, orient, flip):
    count = COUNTS[axis]
    src = pair(nbr_src, axis)
    idx = pair(nbr_idx, axis)
    codes = pair(orient, axis)
    here = jnp.where(src == 1, idx - 256 * axis, -1)
    there = jnp.where(src == 2 + 2 * axis, idx, jnp.where(src == 3 + 2 * axis, idx + count, -1))
    near = pick(lax.broadcasted_iota(jnp.int32, (256, 256), 0) == here)
    far = pick(lax.broadcasted_iota(jnp.int32, (2 * count, 256), 0) == there)
    high, low = split2(planes)
    far_high, far_low = split2(arrived[STARTS[axis] : STARTS[axis] + 2 * count, :].T)
    found = dot(high, near) + dot(low, near) + dot(far_high, far) + dot(far_low, far)
    return reorient(found, codes, flip)


def face_planes(field):
    side = [field[pl.ds(256, 256), :], field[pl.ds(14 * 256, 256), :]]
    middle = [
        jnp.concatenate([field[pl.ds(256 * i + 16 * j, 16), :] for i in range(16)], axis=0) for j in (1, 14)
    ]
    inner = [field[pl.ds(k, 256, stride=16), :] for k in (1, 14)]
    return [jnp.concatenate(both, axis=1) for both in (side, middle, inner)]


def exchange_field_kernel(field, send, arrived_out, msgs, arrived, send_sem, recv_sem):
    me = lax.axis_index("dev")
    make_messages(face_planes(field), send, msgs)
    greet(me)
    for copy in start_copies(me, msgs, arrived, send_sem, recv_sem):
        copy.wait()
    arrived_out[...] = arrived[...]


def exchange_rims_kernel(rims, send, arrived_out, msgs, arrived, send_sem, recv_sem):
    me = lax.axis_index("dev")
    make_messages([rims[axis] for axis in range(3)], send, msgs)
    greet(me)
    for copy in start_copies(me, msgs, arrived, send_sem, recv_sem):
        copy.wait()
    arrived_out[...] = arrived[...]


def make_operators(mats, turned, products, left, right, l1, l2, l4, l5, d12, d0):
    rb = left[0:336, :]
    rc = left[336:672, :]
    ra = left[672:816, :]
    rj = left[816:1136, :]
    rk = left[1136:1456, :]
    cols = lambda n: right[32 * n : 32 * n + 32, :]
    first = deepen(rb, widen(turned[1], cols(0))) * deepen(rc, widen(turned[2], cols(1)))
    high, low = split2(first)
    l1[:, 0:256] = high[:, 0:256]
    l1[:, 256:512] = high[:, 0:256]
    l1[:, 512:768] = low[:, 0:256]
    lane = lax.broadcasted_iota(jnp.int32, (ROWS, 256), 1)
    l1[:, 768:1024] = jnp.where(lane < 128, high[:, 256:].astype(F32), low[:, 256:].astype(F32)).astype(BF)
    lane = lax.broadcasted_iota(jnp.int32, (144, 512), 1)
    row = lax.broadcasted_iota(jnp.int32, (144, 512), 0)
    same = (lane & 7) == (row & 7)
    for mat, out in ((turned[0], l2), (mats[0], l4)):
        whole = jnp.where(same, deepen(ra, widen(mat, cols(2))), 0.0)
        high, low = split2(whole)
        out[...] = jnp.where(lane < 288, high.astype(F32), low.astype(F32)).astype(BF)
    for half in range(2):
        whole = deepen(rj, widen(mats[1], cols(3 + half))) * deepen(rk, widen(mats[2], cols(5 + half)))
        high, low = split2(whole)
        lane = lax.broadcasted_iota(jnp.int32, (RIM, 512), 1) + 512 * half
        l5[:, 512 * half : 512 * half + 512] = jnp.where(
            lane < 2 * ROWS, high.astype(F32), low.astype(F32)
        ).astype(BF)
    d12[...] = deepen(rb, products[1]) + deepen(rc, products[2])
    d0[...] = deepen(ra, products[0])


def solve_kernel(
    field, arrived, nbr_src, nbr_idx, orient, mats, turned, products, left, right, flip_in,
    solved, rims, l1, l2, l4, l5, d12, d0, ghosts, mid,
):
    make_operators(mats, turned, products, left, right, l1, l2, l4, l5, d12, d0)
    flip = flip_in[...]
    planes = face_planes(field)
    for axis in range(3):
        ghosts[axis] = gather(axis, planes[axis], arrived, nbr_src, nbr_idx, orient, flip)

    def forward_edges():
        high, low = split2(ghosts[0])
        out = dot(l1[:, 0:768], jnp.concatenate([high, low, high], axis=0))
        mid[0] = out[:, :SLOTS]
        mid[17] = out[:, SLOTS:]

    forward_edges()

    def forward(t):
        base = pl.multiple_of(512 * t, 512)
        x = jnp.concatenate([field[pl.ds(base, 256), :], field[pl.ds(base + 256, 256), :]], axis=1)
        high, low = split2(x)
        half = pl.multiple_of(32 * t, 32)
        rows = [ghosts[axis, pl.ds(half + 16 * n, 16), :] for axis in (1, 2) for n in (0, 1)]
        extra = jnp.concatenate(
            [
                jnp.concatenate([rows[n][:, :SLOTS], rows[n][:, SLOTS:], rows[n + 2][:, :SLOTS], rows[n + 2][:, SLOTS:]], axis=0)
                for n in (0, 1)
            ],
            axis=1,
        )
        g_high, g_low = split2(extra)
        data = jnp.concatenate([high, low, high, g_high, g_low, g_high, jnp.zeros((64, 256), BF)], axis=0)
        out = dot(l1[...], data)
        mid[2 * t + 1] = out[:, :SLOTS]
        mid[2 * t + 2] = out[:, SLOTS:]

    @pl.loop(0, 4)
    def _(t):
        forward(2 * t)
        forward(2 * t + 1)

    def middle(g):
        start = pl.multiple_of(16 * g, 16)
        block = mid[:, pl.ds(start, 16), :]
        y = jnp.concatenate([block[:, 0:8].reshape(144, SLOTS), block[:, 8:16].reshape(144, SLOTS)], axis=1)
        high, low = split2(y)
        z = dot(l2[:, 0:432], jnp.concatenate([high, low, high], axis=0))
        d = d12[pl.ds(start, 16), :]
        d = jnp.concatenate([d[0:8], d[8:16]], axis=1)
        base = d0[...]
        base = jnp.concatenate([base, base], axis=1)
        z = z / (base + jnp.concatenate([d] * NE, axis=0))
        high, low = split2(z)
        u = dot(l4[:, 0:432], jnp.concatenate([high, low, high], axis=0))
        mid[:, pl.ds(start, 8), :] = u[:, :SLOTS].reshape(NE, 8, SLOTS)
        mid[:, pl.ds(start + 8, 8), :] = u[:, SLOTS:].reshape(NE, 8, SLOTS)

    @pl.loop(0, 7)
    def _(g):
        for n in range(3):
            middle(3 * g + n)

    def spread(first, second):
        u = jnp.concatenate([mid[first], mid[second]], axis=1)
        high, low = split2(u)
        return jnp.concatenate([high, low, high, jnp.zeros((16, 256), BF)], axis=0)

    rims[0] = dot(l5[0:256, :], spread(0, 17))

    def inverse(t):
        out = dot(l5[...], spread(2 * t + 1, 2 * t + 2))
        base = pl.multiple_of(512 * t, 512)
        half = pl.multiple_of(32 * t, 32)
        for n in range(2):
            lanes = slice(SLOTS * n, SLOTS * n + SLOTS)
            solved[pl.ds(base + 256 * n, 256), :] = out[0:256, lanes]
            for axis in (1, 2):
                for side in (0, 1):
                    start = 256 + 32 * (axis - 1) + 16 * side
                    rims[axis, pl.ds(half + 16 * n, 16), SLOTS * side : SLOTS * side + SLOTS] = out[
                        start : start + 16, lanes
                    ]

    @pl.loop(0, 4)
    def _(t):
        inverse(2 * t)
        inverse(2 * t + 1)


def finish_kernel(solved, rims, arrived, nbr_src, nbr_idx, orient, flip_in, out, back):
    flip = flip_in[...]
    for axis in range(3):
        back[axis] = gather(axis, rims[axis], arrived, nbr_src, nbr_idx, orient, flip)
    rank = lax.broadcasted_iota(jnp.int32, (16, 16, SLOTS), 1)

    @pl.loop(0, 16)
    def _(i):
        base = pl.multiple_of(256 * i, 256)
        half = pl.multiple_of(16 * i, 16)
        inner = back[2, pl.ds(half, 16), :]
        low = jnp.broadcast_to(inner[:, None, :SLOTS], (16, 16, SLOTS))
        high = jnp.broadcast_to(inner[:, None, SLOTS:], (16, 16, SLOTS))
        added = jnp.where(rank == 1, low, jnp.where(rank == 14, high, 0.0)).reshape(256, SLOTS)
        out[pl.ds(base, 256), :] = solved[pl.ds(base, 256), :] + added
        out[pl.ds(base + 16, 16), :] += back[1, pl.ds(half, 16), :SLOTS]
        out[pl.ds(base + 224, 16), :] += back[1, pl.ds(half, 16), SLOTS:]

    out[256:512, :] += back[0, :, :SLOTS]
    out[14 * 256 : 15 * 256, :] += back[0, :, SLOTS:]


def exchange(kernel, planes, send, name, number):
    return pl.pallas_call(
        kernel,
        out_shape=jax.ShapeDtypeStruct((192, 256), F32),
        in_specs=[VMEM] * 2,
        out_specs=VMEM,
        scratch_shapes=[
            pltpu.VMEM((192, 256), F32),
            pltpu.VMEM((192, 256), F32),
            pltpu.SemaphoreType.DMA((6,)),
            pltpu.SemaphoreType.DMA((6,)),
        ],
        compiler_params=pltpu.CompilerParams(collective_id=number, has_side_effects=True),
        name=name,
    )(planes, send)


def shards(field, s_mats, lam, coeff, nbr_src, nbr_idx, orient, send_x, send_y, send_z):
    left, right, flip = (jnp.asarray(table, BF) for table in make_tables())
    flat = field.reshape(4096, SLOTS)
    mats = jnp.pad(s_mats, ((0, 0), (0, 14), (0, 14)))
    turned = jnp.swapaxes(mats, 1, 2)
    products = jnp.pad(lam[:, :, None] * coeff[:, None, :], ((0, 0), (0, 14), (0, 0)))
    blank = ((0, 0), (0, 96))
    send = jnp.concatenate(
        [
            jnp.pad(send_x.reshape(1, 32), blank, constant_values=-1),
            jnp.pad(send_y.reshape(1, 32), blank, constant_values=-1),
            send_z.reshape(1, SLOTS),
        ],
        axis=0,
    )
    arrived = exchange(exchange_field_kernel, flat, send, "exchange_field", 0)
    solved, rims = pl.pallas_call(
        solve_kernel,
        out_shape=(jax.ShapeDtypeStruct((4096, SLOTS), F32), jax.ShapeDtypeStruct((3, 256, 256), F32)),
        in_specs=[VMEM] * 11,
        out_specs=(VMEM, VMEM),
        scratch_shapes=[
            pltpu.VMEM((ROWS, 1024), BF),
            pltpu.VMEM((144, 512), BF),
            pltpu.VMEM((144, 512), BF),
            pltpu.VMEM((RIM, 1024), BF),
            pltpu.VMEM((ROWS, SLOTS), F32),
            pltpu.VMEM((144, SLOTS), F32),
            pltpu.VMEM((3, 256, 256), F32),
            pltpu.VMEM((NE, ROWS, SLOTS), F32),
        ],
        name="solve",
    )(flat, arrived, nbr_src, nbr_idx, orient, mats, turned, products, left, right, flip)
    returned = exchange(exchange_rims_kernel, rims, send, "exchange_rims", 1)
    out = pl.pallas_call(
        finish_kernel,
        out_shape=jax.ShapeDtypeStruct((4096, SLOTS), F32),
        in_specs=[VMEM] * 7,
        out_specs=VMEM,
        scratch_shapes=[pltpu.VMEM((3, 256, 256), F32)],
        name="finish",
    )(solved, rims, returned, nbr_src, nbr_idx, orient, flip)
    return out.reshape(field.shape)


def solution(mesh):
    placed = (
        P(None, None, None, "dev"),
        P(),
        P(),
        P(None, "dev"),
        P(None, "dev"),
        P(None, "dev"),
        P(None, "dev"),
        P(None, "dev"),
        P(None, "dev"),
        P(None, "dev"),
    )
    return jax.shard_map(
        shards, mesh=mesh, in_specs=placed, out_specs=P(None, None, None, "dev"), check_vma=False
    )
```

```python
import functools

import jax
import jax.numpy as jnp
import numpy as np
from jax import lax
from jax.experimental import pallas as pl
from jax.experimental.pallas import tpu as pltpu
from jax.sharding import PartitionSpec as P

NP = 16
NE = 18
SLOTS = 128
ROWS = 336
RIM = 320
COUNTS = (16, 16, 64)
STARTS = (0, 32, 64)
OFFSETS = (-1, 1, -4, 4, -16, 16)
BF = jnp.bfloat16
F32 = jnp.float32
VMEM = pl.BlockSpec(memory_space=pltpu.VMEM)


def make_tables():
    r = np.arange(ROWS)
    fits = r < NE * NE
    rb = np.zeros((ROWS, 96))
    rc = np.zeros((ROWS, 96))
    ra = np.zeros((NE * 8, 96))
    for t in range(3):
        rb[r[fits], t * 32 + r[fits] // NE] = 1
        rc[r[fits], t * 32 + r[fits] % NE] = 1
        ra[np.arange(NE * 8), t * 32 + np.arange(NE * 8) // 8] = 1
    inner = np.arange(1, 17)
    low, high = np.zeros(16, int), np.full(16, 17)
    jq = np.concatenate([np.repeat(inner, 16), low, high, inner, inner])
    kq = np.concatenate([np.tile(inner, 16), inner, inner, low, high])
    rj = np.zeros((RIM, 96))
    rk = np.zeros((RIM, 96))
    for t in range(3):
        rj[np.arange(RIM), t * 32 + jq] = 1
        rk[np.arange(RIM), t * 32 + kq] = 1
    cols = np.concatenate([np.arange(256), np.tile(np.arange(256, 320), 3)])
    qj = np.zeros((32, 512))
    qk = np.zeros((32, 512))
    qj[jq[cols], np.arange(448)] = 1
    qk[kq[cols], np.arange(448)] = 1
    qi = np.zeros((32, 512))
    c = np.arange(432)
    qi[(c % 144) // 8, c] = 1
    qb = np.zeros((32, 1024))
    qc = np.zeros((32, 1024))
    c = np.arange(1008)
    c = c[c % ROWS < NE * NE]
    qb[c % ROWS // NE, c] = 1
    qc[c % ROWS % NE, c] = 1
    left = np.concatenate([rb, rc, ra, rj, rk])
    right = np.concatenate([qj, qk, qi, qb[:, :512], qb[:, 512:], qc[:, :512], qc[:, 512:]])
    return left, right


def split2(x):
    high = x.astype(BF)
    return high, (x - high.astype(F32)).astype(BF)


def split3(x):
    high = x.astype(BF)
    rest = x - high.astype(F32)
    middle = rest.astype(BF)
    return high, middle, (rest - middle.astype(F32)).astype(BF)


def dot(a, b):
    return jnp.dot(a, b, preferred_element_type=F32)


def widen(small, right):
    return sum(dot(term, right) for term in split3(small))


def deepen(left, small):
    return dot(left, jnp.concatenate(split3(small), axis=0))


def pick(condition):
    return jnp.where(condition, 1.0, 0.0).astype(BF)


def list_rows(direction):
    axis, side = direction // 2, direction % 2
    return STARTS[axis] + side * COUNTS[axis], COUNTS[axis]


def find_neighbours(me):
    spot = (lax.rem(me, 4), lax.rem(lax.div(me, 4), 4), lax.div(me, 16))
    tops = (3, 3, 15)
    return [spot[d // 2] > 0 if d % 2 == 0 else spot[d // 2] < tops[d // 2] for d in range(6)]


def greet(me, present):
    barrier = pltpu.get_barrier_semaphore()
    for direction in range(6):

        @pl.when(present[direction])
        def _():
            pl.semaphore_signal(
                barrier, inc=1, device_id=(me + OFFSETS[direction],), device_id_type=pl.DeviceIdType.MESH
            )

    return barrier


def outgoing(me, direction, msgs, arrived, send_sem, recv_sem):
    start, count = list_rows(direction)
    return pltpu.make_async_remote_copy(
        src_ref=msgs.at[pl.ds(start, count)],
        dst_ref=arrived.at[pl.ds(start, count)],
        send_sem=send_sem.at[direction],
        recv_sem=recv_sem.at[direction],
        device_id=(me + OFFSETS[direction],),
        device_id_type=pl.DeviceIdType.MESH,
    )


def send_axis(axis, me, present, parts, send, msgs, arrived, send_sem, recv_sem):
    count = 2 * COUNTS[axis]
    ids = send[axis : axis + 1, :] - 256 * axis
    chosen = pick(lax.broadcasted_iota(jnp.int32, (256, SLOTS), 0) == ids)
    found = dot(parts[axis, 0], chosen) + dot(parts[axis, 1], chosen)
    msgs[STARTS[axis] : STARTS[axis] + count, :] = found.T[:count]


def launch(axis, me, present, msgs, arrived, send_sem, recv_sem):
    for direction in (2 * axis, 2 * axis + 1):

        @pl.when(present[direction])
        def _():
            outgoing(me, direction, msgs, arrived, send_sem, recv_sem).start()


def await_axis(axis, me, present, msgs, arrived, send_sem, recv_sem):
    for direction in (2 * axis, 2 * axis + 1):

        @pl.when(present[direction])
        def _():
            outgoing(me, direction, msgs, arrived, send_sem, recv_sem).wait_send()

        @pl.when(present[direction ^ 1])
        def _():
            outgoing(me, direction, msgs, arrived, send_sem, recv_sem).wait_recv()


def pair(table, axis):
    return jnp.concatenate([table[2 * axis : 2 * axis + 1, :], table[2 * axis + 1 : 2 * axis + 2, :]], axis=1)


def gather_near(axis, parts, found, nbr_src, nbr_idx):
    src = pair(nbr_src, axis)
    idx = pair(nbr_idx, axis)
    here = jnp.where(src == 1, idx - 256 * axis, -1)
    near = pick(lax.broadcasted_iota(jnp.int32, (256, 256), 0) == here)
    found[axis] = dot(parts[axis, 0], near) + dot(parts[axis, 1], near)


def gather_far(axis, arrived, found, out, nbr_src, nbr_idx, orient):
    count = COUNTS[axis]
    src = pair(nbr_src, axis)
    idx = pair(nbr_idx, axis)
    codes = pair(orient, axis)
    there = jnp.where(src == 2 + 2 * axis, idx, jnp.where(src == 3 + 2 * axis, idx + count, -1))
    far = pick(lax.broadcasted_iota(jnp.int32, (2 * count, 256), 0) == there)
    high, low = split2(arrived[STARTS[axis] : STARTS[axis] + 2 * count, :].T)
    found[axis] += dot(high, far) + dot(low, far)
    first = codes % 2 == 1
    second = codes >= 2
    back = 7 - lax.broadcasted_iota(jnp.int32, (8, SLOTS), 0)
    for lanes in (slice(0, SLOTS), slice(SLOTS, 2 * SLOTS)):
        for u in range(16):
            rows = [
                jnp.where(
                    first[:, lanes],
                    found[axis, 16 * (15 - u) + 8 * n : 16 * (15 - u) + 8 * n + 8, lanes],
                    found[axis, 16 * u + 8 * n : 16 * u + 8 * n + 8, lanes],
                )
                for n in (0, 1)
            ]
            for n in (0, 1):
                turned = jnp.take_along_axis(rows[1 - n], back, axis=0)
                out[axis, 16 * u + 8 * n : 16 * u + 8 * n + 8, lanes] = jnp.where(second[:, lanes], turned, rows[n])


def face_planes(axis, field):
    if axis == 0:
        both = [field[256:512, :], field[14 * 256 : 15 * 256, :]]
    elif axis == 1:
        both = [
            jnp.concatenate([field[256 * i + 16 * j : 256 * i + 16 * j + 16, :] for i in range(16)], axis=0)
            for j in (1, 14)
        ]
    else:
        both = [field[pl.ds(k, 256, stride=16), :] for k in (1, 14)]
    return jnp.concatenate(both, axis=1)


def product_blocks(rows, depth, left_a, left_b, small_a, small_b, columns):
    split_a = jnp.concatenate(split3(small_a), axis=0)
    split_b = jnp.concatenate(split3(small_b), axis=0)
    for start in range(0, rows, depth):
        piece = slice(start, start + depth)
        yield piece, dot(left_a[piece, :], split_a[:, columns]) * dot(left_b[piece, :], split_b[:, columns])


def make_operators(s_mats, lam, coeff, left, right, l1, l2, l4, l5, d12, d0):
    rb = left.at[0:336]
    rc = left.at[336:672]
    ra = left.at[672:816]
    rj = left.at[816:1136]
    rk = left.at[1136:1456]
    cols = lambda n: right[32 * n : 32 * n + 32, :]
    room = ((0, 14), (0, 14))
    mats = [jnp.pad(s_mats[axis], room) for axis in range(3)]
    turned = [jnp.pad(s_mats[axis].T, room) for axis in range(3)]
    small = widen(turned[1], cols(0)), widen(turned[2], cols(1))
    for piece, block in product_blocks(ROWS, 112, rb, rc, *small, slice(0, 256)):
        high, low = split2(block)
        l1[piece, 0:256] = high
        l1[piece, 256:512] = high
        l1[piece, 512:768] = low
    lane = lax.broadcasted_iota(jnp.int32, (112, 256), 1)
    for piece, block in product_blocks(ROWS, 112, rb, rc, *small, slice(256, 512)):
        high, low = split2(block)
        l1[piece, 768:1024] = jnp.where(lane < 128, high.astype(F32), low.astype(F32)).astype(BF)
    lane = lax.broadcasted_iota(jnp.int32, (144, 256), 1)
    row = lax.broadcasted_iota(jnp.int32, (144, 256), 0)
    same = (lane & 7) == (row & 7)
    for mat, out in ((turned[0], l2), (mats[0], l4)):
        whole = jnp.concatenate(split3(widen(mat, cols(2))), axis=0)
        for half in range(2):
            columns = slice(256 * half, 256 * half + 256)
            high, low = split2(jnp.where(same, dot(ra[...], whole[:, columns]), 0.0))
            out[:, columns] = jnp.where(lane < 288 - 256 * half, high.astype(F32), low.astype(F32)).astype(BF)
    lane = lax.broadcasted_iota(jnp.int32, (80, 256), 1)
    for half in range(2):
        small = widen(mats[1], cols(3 + half)), widen(mats[2], cols(5 + half))
        for part in range(2):
            base = 512 * half + 256 * part
            for piece, block in product_blocks(RIM, 80, rj, rk, *small, slice(256 * part, 256 * part + 256)):
                high, low = split2(block)
                l5[piece, base : base + 256] = jnp.where(
                    lane < 2 * ROWS - base, high.astype(F32), low.astype(F32)
                ).astype(BF)
    levels = jnp.pad(lam[...], ((0, 5), (0, 110))).T[:32]
    products = [levels[:, axis : axis + 1] * coeff[axis : axis + 1, :] for axis in range(3)]
    d12[...] = deepen(rb[...], products[1]) + deepen(rc[...], products[2])
    d0[...] = deepen(ra[...], products[0])


def smooth_kernel(
    field_in, s_mats_in, lam_in, coeff_in, src_in, idx_in, orient_in, send_x_in, send_y_in, send_z_in, left_in, right_in,
    solved_out, back_out,
    field, s_mats, lam, coeff, nbr_src, nbr_idx, orient, send_x, send_y, send_z, left, right,
    l1, l2, l4, l5, d12, d0, send, parts, found, ghosts, mid, solved,
    msgs, arrived, load_sem, store_sem, send_sem, recv_sem,
):
    me = lax.axis_index("dev")
    loads = [
        pltpu.make_async_copy(source, target, load_sem.at[n])
        for n, (source, target) in enumerate(
            (
                (field_in, field), (send_x_in, send_x), (send_y_in, send_y), (send_z_in, send_z),
                (left_in, left), (right_in, right), (s_mats_in, s_mats), (lam_in, lam), (coeff_in, coeff),
                (src_in, nbr_src), (idx_in, nbr_idx), (orient_in, orient),
            )
        )
    ]
    for load in loads:
        load.start()
    present = find_neighbours(me)
    for direction in range(6):
        start, count = list_rows(direction)

        @pl.when(jnp.logical_not(present[direction ^ 1]))
        def _():
            for phase in range(2):
                arrived[phase, start : start + count, :] = jnp.zeros((count, 256), F32)

    barrier = greet(me, present)
    for load in loads[:4]:
        load.wait()
    send[...] = jnp.full((8, SLOTS), -1, jnp.int32)
    send[0:1, 0:16] = send_x[0:1, :]
    send[0:1, 16:32] = send_x[1:2, :]
    send[1:2, 0:16] = send_y[0:1, :]
    send[1:2, 16:32] = send_y[1:2, :]
    send[2:3, 0:64] = send_z[0:1, :]
    send[2:3, 64:128] = send_z[1:2, :]

    wires = [(me, present, msgs, arrived.at[n], send_sem.at[n], recv_sem.at[n]) for n in range(2)]

    def send_planes(axis, wire):
        send_axis(axis, *wire[:2], parts, send, *wire[2:])

    for axis in (2, 0, 1):
        parts[axis, 0], parts[axis, 1] = split2(face_planes(axis, field))
        send_planes(axis, wires[0])
        if axis == 2:
            total = sum(jnp.where(flag, 1, 0) for flag in present)
            pl.semaphore_wait(barrier, total)
        launch(axis, *wires[0])

    for load in loads[4:]:
        load.wait()
    make_operators(s_mats, lam, coeff, left, right, l1, l2, l4, l5, d12, d0)
    for axis in range(3):
        gather_near(axis, parts, found, nbr_src, nbr_idx)

    def forward_inner(t):
        base = pl.multiple_of(512 * t, 512)
        x = jnp.concatenate([field[pl.ds(base, 256), :], field[pl.ds(base + 256, 256), :]], axis=1)
        high, low = split2(x)
        out = dot(l1[:, 0:768], jnp.concatenate([high, low, high], axis=0))
        mid[2 * t + 1] = out[:, :SLOTS]
        mid[2 * t + 2] = out[:, SLOTS:]

    @pl.loop(0, 4)
    def _(t):
        forward_inner(2 * t)
        forward_inner(2 * t + 1)

    for axis in (0, 1, 2):
        await_axis(axis, *wires[0])
        gather_far(axis, arrived.at[0], found, ghosts, nbr_src, nbr_idx, orient)

    high, low = split2(ghosts[0])
    out = dot(l1[:, 0:768], jnp.concatenate([high, low, high], axis=0))
    mid[0] = out[:, :SLOTS]
    mid[17] = out[:, SLOTS:]

    def forward_outer(t):
        half = pl.multiple_of(32 * t, 32)
        extra = jnp.concatenate(
            [
                jnp.concatenate(
                    [
                        ghosts[axis, pl.ds(half + 16 * n, 16), SLOTS * side : SLOTS * side + SLOTS]
                        for axis in (1, 2)
                        for side in (0, 1)
                    ],
                    axis=0,
                )
                for n in (0, 1)
            ],
            axis=1,
        )
        high, low = split2(extra)
        out = dot(l1[:, 768:960], jnp.concatenate([high, low, high], axis=0))
        mid[2 * t + 1] += out[:, :SLOTS]
        mid[2 * t + 2] += out[:, SLOTS:]

    @pl.loop(0, 4)
    def _(t):
        forward_outer(2 * t)
        forward_outer(2 * t + 1)

    def middle(g):
        start = pl.multiple_of(16 * g, 16)
        block = mid[:, pl.ds(start, 16), :]
        y = jnp.concatenate([block[:, 0:8].reshape(144, SLOTS), block[:, 8:16].reshape(144, SLOTS)], axis=1)
        high, low = split2(y)
        z = dot(l2[:, 0:432], jnp.concatenate([high, low, high], axis=0))
        d = d12[pl.ds(start, 16), :]
        d = jnp.concatenate([d[0:8], d[8:16]], axis=1)
        base = d0[...]
        base = jnp.concatenate([base, base], axis=1)
        z = z / (base + jnp.concatenate([d] * NE, axis=0))
        high, low = split2(z)
        u = dot(l4[:, 0:432], jnp.concatenate([high, low, high], axis=0))
        mid[:, pl.ds(start, 8), :] = u[:, :SLOTS].reshape(NE, 8, SLOTS)
        mid[:, pl.ds(start + 8, 8), :] = u[:, SLOTS:].reshape(NE, 8, SLOTS)

    @pl.loop(0, 7)
    def _(g):
        for n in range(3):
            middle(3 * g + n)

    def spread(first, second):
        u = jnp.concatenate([mid[first], mid[second]], axis=1)
        high, low = split2(u)
        return jnp.concatenate([high, low, high, jnp.zeros((16, 256), BF)], axis=0)

    parts[0, 0], parts[0, 1] = split2(dot(l5[0:256, :], spread(0, 17)))
    send_planes(0, wires[1])
    launch(0, *wires[1])

    def store(t):
        rows = pl.ds(pl.multiple_of(512 * t, 512), 512)
        return pltpu.make_async_copy(solved.at[rows], solved_out.at[rows], store_sem.at[t])

    def inverse(t):
        out = dot(l5[...], spread(2 * t + 1, 2 * t + 2))
        base = pl.multiple_of(512 * t, 512)
        half = pl.multiple_of(32 * t, 32)
        for n in range(2):
            lanes = slice(SLOTS * n, SLOTS * n + SLOTS)
            solved[pl.ds(base + 256 * n, 256), :] = out[0:256, lanes]
            for axis in (1, 2):
                for side in (0, 1):
                    start = 256 + 32 * (axis - 1) + 16 * side
                    high, low = split2(out[start : start + 16, lanes])
                    rows = pl.ds(half + 16 * n, 16)
                    parts[axis, 0, rows, SLOTS * side : SLOTS * side + SLOTS] = high
                    parts[axis, 1, rows, SLOTS * side : SLOTS * side + SLOTS] = low

    @pl.loop(0, 4)
    def _(t):
        inverse(2 * t)
        inverse(2 * t + 1)

    for axis in (2, 1):
        send_planes(axis, wires[1])
        launch(axis, *wires[1])
    for t in range(8):
        store(t).start()
    for axis in range(3):
        gather_near(axis, parts, found, nbr_src, nbr_idx)
    for axis in (0, 1, 2):
        await_axis(axis, *wires[1])
        gather_far(axis, arrived.at[1], found, back_out, nbr_src, nbr_idx, orient)
    for t in range(8):
        store(t).wait()


def finish_kernel(solved, back, out):
    step = pl.program_id(0)
    rank = lax.broadcasted_iota(jnp.int32, (16, 16, SLOTS), 1)
    for n in range(2):
        half = pl.multiple_of(32 * step + 16 * n, 16)
        base = 256 * n
        inner = back[2, pl.ds(half, 16), :]
        low = jnp.broadcast_to(inner[:, None, :SLOTS], (16, 16, SLOTS))
        high = jnp.broadcast_to(inner[:, None, SLOTS:], (16, 16, SLOTS))
        added = jnp.where(rank == 1, low, jnp.where(rank == 14, high, 0.0)).reshape(256, SLOTS)
        out[base : base + 256, :] = solved[base : base + 256, :] + added
        out[base + 16 : base + 32, :] += back[1, pl.ds(half, 16), :SLOTS]
        out[base + 224 : base + 240, :] += back[1, pl.ds(half, 16), SLOTS:]

    @pl.when(step == 0)
    def _():
        out[256:512, :] += back[0, :, :SLOTS]

    @pl.when(step == 7)
    def _():
        out[0:256, :] += back[0, :, SLOTS:]


def shards(field, s_mats, lam, coeff, nbr_src, nbr_idx, orient, send_x, send_y, send_z):
    left, right = (jnp.asarray(table, BF) for table in make_tables())
    flat = field.reshape(4096, SLOTS)
    inputs = (flat, s_mats, lam, coeff, nbr_src, nbr_idx, orient, send_x, send_y, send_z, left, right)
    solved, back = pl.pallas_call(
        smooth_kernel,
        out_shape=(jax.ShapeDtypeStruct((4096, SLOTS), F32), jax.ShapeDtypeStruct((3, 256, 256), F32)),
        in_specs=[pl.BlockSpec(memory_space=pl.ANY)] * 12,
        out_specs=(pl.BlockSpec(memory_space=pl.ANY), VMEM),
        scratch_shapes=[pltpu.VMEM(value.shape, value.dtype) for value in inputs]
        + [
            pltpu.VMEM((ROWS, 1024), BF),
            pltpu.VMEM((144, 512), BF),
            pltpu.VMEM((144, 512), BF),
            pltpu.VMEM((RIM, 1024), BF),
            pltpu.VMEM((ROWS, SLOTS), F32),
            pltpu.VMEM((144, SLOTS), F32),
            pltpu.VMEM((8, SLOTS), jnp.int32),
            pltpu.VMEM((3, 2, 256, 256), BF),
            pltpu.VMEM((3, 256, 256), F32),
            pltpu.VMEM((3, 256, 256), F32),
            pltpu.VMEM((NE, ROWS, SLOTS), F32),
            pltpu.VMEM((4096, SLOTS), F32),
            pltpu.VMEM((192, 256), F32),
            pltpu.VMEM((2, 192, 256), F32),
            pltpu.SemaphoreType.DMA((12,)),
            pltpu.SemaphoreType.DMA((8,)),
            pltpu.SemaphoreType.DMA((2, 6)),
            pltpu.SemaphoreType.DMA((2, 6)),
        ],
        compiler_params=pltpu.CompilerParams(collective_id=0, has_side_effects=True),
        name="smooth",
    )(*inputs)
    whole = lambda step: (0, 0, 0)
    some = pl.BlockSpec((512, SLOTS), lambda step: (step, 0))
    out = pl.pallas_call(
        finish_kernel,
        out_shape=jax.ShapeDtypeStruct((4096, SLOTS), F32),
        grid=(8,),
        in_specs=[some, pl.BlockSpec((3, 256, 256), whole)],
        out_specs=some,
        name="finish",
    )(solved, back)
    return out.reshape(field.shape)


def solution(mesh):
    placed = (
        P(None, None, None, "dev"),
        P(),
        P(),
        P(None, "dev"),
        P(None, "dev"),
        P(None, "dev"),
        P(None, "dev"),
        P(None, "dev"),
        P(None, "dev"),
        P(None, "dev"),
    )
    return jax.shard_map(
        shards, mesh=mesh, in_specs=placed, out_specs=P(None, None, None, "dev"), check_vma=False
    )
```

```python
import functools

import jax
import jax.numpy as jnp
import numpy as np
from jax import lax
from jax.experimental import pallas as pl
from jax.experimental.pallas import tpu as pltpu
from jax.sharding import PartitionSpec as P

NP = 16
NE = 18
SLOTS = 128
ROWS = 336
RIM = 320
COUNTS = (16, 16, 64)
STARTS = (0, 32, 64)
OFFSETS = (-1, 1, -4, 4, -16, 16)
BF = jnp.bfloat16
F32 = jnp.float32
VMEM = pl.BlockSpec(memory_space=pltpu.VMEM)


def make_tables():
    r = np.arange(ROWS)
    fits = r < NE * NE
    rb = np.zeros((ROWS, 96))
    rc = np.zeros((ROWS, 96))
    ra = np.zeros((NE * 8, 96))
    for t in range(3):
        rb[r[fits], t * 32 + r[fits] // NE] = 1
        rc[r[fits], t * 32 + r[fits] % NE] = 1
        ra[np.arange(NE * 8), t * 32 + np.arange(NE * 8) // 8] = 1
    inner = np.arange(1, 17)
    low, high = np.zeros(16, int), np.full(16, 17)
    jq = np.concatenate([np.repeat(inner, 16), low, high, inner, inner])
    kq = np.concatenate([np.tile(inner, 16), inner, inner, low, high])
    rj = np.zeros((RIM, 96))
    rk = np.zeros((RIM, 96))
    for t in range(3):
        rj[np.arange(RIM), t * 32 + jq] = 1
        rk[np.arange(RIM), t * 32 + kq] = 1
    cols = np.concatenate([np.arange(256), np.tile(np.arange(256, 320), 3)])
    qj = np.zeros((32, 512))
    qk = np.zeros((32, 512))
    qj[jq[cols], np.arange(448)] = 1
    qk[kq[cols], np.arange(448)] = 1
    qi = np.zeros((32, 512))
    c = np.arange(432)
    qi[(c % 144) // 8, c] = 1
    qb = np.zeros((32, 1024))
    qc = np.zeros((32, 1024))
    c = np.arange(1008)
    c = c[c % ROWS < NE * NE]
    qb[c % ROWS // NE, c] = 1
    qc[c % ROWS % NE, c] = 1
    left = np.concatenate([rb, rc, ra, rj, rk])
    right = np.concatenate([qj, qk, qi, qb[:, :512], qb[:, 512:], qc[:, :512], qc[:, 512:]])
    return left, right


def split2(x):
    high = x.astype(BF)
    return high, (x - high.astype(F32)).astype(BF)


def split3(x):
    high = x.astype(BF)
    rest = x - high.astype(F32)
    middle = rest.astype(BF)
    return high, middle, (rest - middle.astype(F32)).astype(BF)


def dot(a, b):
    return jnp.dot(a, b, preferred_element_type=F32)


def widen(small, right):
    return sum(dot(term, right) for term in split3(small))


def deepen(left, small):
    return dot(left, jnp.concatenate(split3(small), axis=0))


def pick(condition):
    return jnp.where(condition, 1.0, 0.0).astype(BF)


def aligned(index, step):
    return index if isinstance(index, int) else pl.multiple_of(index, step)


def list_rows(direction):
    axis, side = direction // 2, direction % 2
    return STARTS[axis] + side * COUNTS[axis], COUNTS[axis]


def find_neighbours(me):
    spot = (lax.rem(me, 4), lax.rem(lax.div(me, 4), 4), lax.div(me, 16))
    tops = (3, 3, 15)
    return [spot[d // 2] > 0 if d % 2 == 0 else spot[d // 2] < tops[d // 2] for d in range(6)]


def greet(me, present):
    barrier = pltpu.get_barrier_semaphore()
    for direction in range(6):

        @pl.when(present[direction])
        def _():
            pl.semaphore_signal(
                barrier, inc=1, device_id=(me + OFFSETS[direction],), device_id_type=pl.DeviceIdType.MESH
            )

    return barrier


def outgoing(me, direction, msgs, arrived, send_sem, recv_sem):
    start, count = list_rows(direction)
    return pltpu.make_async_remote_copy(
        src_ref=msgs.at[pl.ds(start, count)],
        dst_ref=arrived.at[pl.ds(start, count)],
        send_sem=send_sem.at[direction],
        recv_sem=recv_sem.at[direction],
        device_id=(me + OFFSETS[direction],),
        device_id_type=pl.DeviceIdType.MESH,
    )


def send_axis(axis, me, present, parts, send, msgs, arrived, send_sem, recv_sem):
    count = 2 * COUNTS[axis]
    ids = send[axis : axis + 1, :] - 256 * axis
    chosen = pick(lax.broadcasted_iota(jnp.int32, (256, SLOTS), 0) == ids)
    found = dot(parts[axis, 0], chosen) + dot(parts[axis, 1], chosen)
    msgs[STARTS[axis] : STARTS[axis] + count, :] = found.T[:count]


def launch(axis, me, present, msgs, arrived, send_sem, recv_sem):
    for direction in (2 * axis, 2 * axis + 1):

        @pl.when(present[direction])
        def _():
            outgoing(me, direction, msgs, arrived, send_sem, recv_sem).start()


def await_axis(axis, me, present, msgs, arrived, send_sem, recv_sem):
    for direction in (2 * axis, 2 * axis + 1):

        @pl.when(present[direction])
        def _():
            outgoing(me, direction, msgs, arrived, send_sem, recv_sem).wait_send()

        @pl.when(present[direction ^ 1])
        def _():
            outgoing(me, direction, msgs, arrived, send_sem, recv_sem).wait_recv()


def pair(table, axis):
    return jnp.concatenate([table[2 * axis : 2 * axis + 1, :], table[2 * axis + 1 : 2 * axis + 2, :]], axis=1)


def gather_near(axis, parts, found, nbr_src, nbr_idx):
    src = pair(nbr_src, axis)
    idx = pair(nbr_idx, axis)
    here = jnp.where(src == 1, idx - 256 * axis, -1)
    near = pick(lax.broadcasted_iota(jnp.int32, (256, 256), 0) == here)
    found[axis] = dot(parts[axis, 0], near) + dot(parts[axis, 1], near)


def gather_far(axis, arrived, found, out, nbr_src, nbr_idx, orient):
    count = COUNTS[axis]
    src = pair(nbr_src, axis)
    idx = pair(nbr_idx, axis)
    codes = pair(orient, axis)
    there = jnp.where(src == 2 + 2 * axis, idx, jnp.where(src == 3 + 2 * axis, idx + count, -1))
    far = pick(lax.broadcasted_iota(jnp.int32, (2 * count, 256), 0) == there)
    high, low = split2(arrived[STARTS[axis] : STARTS[axis] + 2 * count, :].T)
    found[axis] += dot(high, far) + dot(low, far)
    first = codes % 2 == 1
    second = codes >= 2
    back = 7 - lax.broadcasted_iota(jnp.int32, (8, SLOTS), 0)
    for lanes in (slice(0, SLOTS), slice(SLOTS, 2 * SLOTS)):
        for u in range(16):
            rows = [
                jnp.where(
                    first[:, lanes],
                    found[axis, 16 * (15 - u) + 8 * n : 16 * (15 - u) + 8 * n + 8, lanes],
                    found[axis, 16 * u + 8 * n : 16 * u + 8 * n + 8, lanes],
                )
                for n in (0, 1)
            ]
            for n in (0, 1):
                turned = jnp.take_along_axis(rows[1 - n], back, axis=0)
                out[axis, 16 * u + 8 * n : 16 * u + 8 * n + 8, lanes] = jnp.where(second[:, lanes], turned, rows[n])


def face_planes(axis, field):
    if axis == 0:
        both = [field[256:512, :], field[14 * 256 : 15 * 256, :]]
    elif axis == 1:
        both = [
            jnp.concatenate([field[256 * i + 16 * j : 256 * i + 16 * j + 16, :] for i in range(16)], axis=0)
            for j in (1, 14)
        ]
    else:
        both = [field[pl.ds(k, 256, stride=16), :] for k in (1, 14)]
    return jnp.concatenate(both, axis=1)


def product_blocks(rows, depth, left_a, left_b, small_a, small_b, columns):
    split_a = jnp.concatenate(split3(small_a), axis=0)
    split_b = jnp.concatenate(split3(small_b), axis=0)
    for start in range(0, rows, depth):
        piece = slice(start, start + depth)
        yield piece, dot(left_a[piece, :], split_a[:, columns]) * dot(left_b[piece, :], split_b[:, columns])


def make_operators(s_mats, lam, coeff, left, right, l1, l2, l4, l5, d12, d0):
    rb = left.at[0:336]
    rc = left.at[336:672]
    ra = left.at[672:816]
    rj = left.at[816:1136]
    rk = left.at[1136:1456]
    cols = lambda n: right[32 * n : 32 * n + 32, :]
    room = ((0, 14), (0, 14))
    mats = [jnp.pad(s_mats[axis], room) for axis in range(3)]
    turned = [jnp.pad(s_mats[axis].T, room) for axis in range(3)]
    small = widen(turned[1], cols(0)), widen(turned[2], cols(1))
    for piece, block in product_blocks(ROWS, 112, rb, rc, *small, slice(0, 256)):
        high, low = split2(block)
        l1[piece, 0:256] = high
        l1[piece, 256:512] = high
        l1[piece, 512:768] = low
    lane = lax.broadcasted_iota(jnp.int32, (112, 256), 1)
    for piece, block in product_blocks(ROWS, 112, rb, rc, *small, slice(256, 512)):
        high, low = split2(block)
        l1[piece, 768:1024] = jnp.where(lane < 128, high.astype(F32), low.astype(F32)).astype(BF)
    lane = lax.broadcasted_iota(jnp.int32, (144, 256), 1)
    row = lax.broadcasted_iota(jnp.int32, (144, 256), 0)
    same = (lane & 7) == (row & 7)
    for mat, out in ((turned[0], l2), (mats[0], l4)):
        whole = jnp.concatenate(split3(widen(mat, cols(2))), axis=0)
        for half in range(2):
            columns = slice(256 * half, 256 * half + 256)
            high, low = split2(jnp.where(same, dot(ra[...], whole[:, columns]), 0.0))
            out[:, columns] = jnp.where(lane < 288 - 256 * half, high.astype(F32), low.astype(F32)).astype(BF)
    lane = lax.broadcasted_iota(jnp.int32, (80, 256), 1)
    for half in range(2):
        small = widen(mats[1], cols(3 + half)), widen(mats[2], cols(5 + half))
        for part in range(2):
            base = 512 * half + 256 * part
            for piece, block in product_blocks(RIM, 80, rj, rk, *small, slice(256 * part, 256 * part + 256)):
                high, low = split2(block)
                l5[piece, base : base + 256] = jnp.where(
                    lane < 2 * ROWS - base, high.astype(F32), low.astype(F32)
                ).astype(BF)
    levels = jnp.pad(lam[...], ((0, 5), (0, 110))).T[:32]
    products = [levels[:, axis : axis + 1] * coeff[axis : axis + 1, :] for axis in range(3)]
    d12[...] = deepen(rb[...], products[1]) + deepen(rc[...], products[2])
    d0[...] = deepen(ra[...], products[0])


def smooth_kernel(
    field_in, s_mats_in, lam_in, coeff_in, src_in, idx_in, orient_in, send_x_in, send_y_in, send_z_in, left_in, right_in,
    solved,
    field, s_mats, lam, coeff, nbr_src, nbr_idx, orient, send_x, send_y, send_z, left, right,
    l1, l2, l4, l5, d12, d0, send, parts, found, ghosts, mid,
    msgs, arrived, load_sem, send_sem, recv_sem,
):
    me = lax.axis_index("dev")
    loads = [
        pltpu.make_async_copy(source, target, load_sem.at[n])
        for n, (source, target) in enumerate(
            (
                (field_in, field), (send_x_in, send_x), (send_y_in, send_y), (send_z_in, send_z),
                (left_in, left), (right_in, right), (s_mats_in, s_mats), (lam_in, lam), (coeff_in, coeff),
                (src_in, nbr_src), (idx_in, nbr_idx), (orient_in, orient),
            )
        )
    ]
    for load in loads:
        load.start()
    present = find_neighbours(me)
    for direction in range(6):
        start, count = list_rows(direction)

        @pl.when(jnp.logical_not(present[direction ^ 1]))
        def _():
            for phase in range(2):
                arrived[phase, start : start + count, :] = jnp.zeros((count, 256), F32)

    barrier = greet(me, present)
    for load in loads[:4]:
        load.wait()
    send[...] = jnp.full((8, SLOTS), -1, jnp.int32)
    send[0:1, 0:16] = send_x[0:1, :]
    send[0:1, 16:32] = send_x[1:2, :]
    send[1:2, 0:16] = send_y[0:1, :]
    send[1:2, 16:32] = send_y[1:2, :]
    send[2:3, 0:64] = send_z[0:1, :]
    send[2:3, 64:128] = send_z[1:2, :]

    wires = [(me, present, msgs, arrived.at[n], send_sem.at[n], recv_sem.at[n]) for n in range(2)]

    def send_planes(axis, wire):
        send_axis(axis, *wire[:2], parts, send, *wire[2:])

    for axis in (2, 0, 1):
        parts[axis, 0], parts[axis, 1] = split2(face_planes(axis, field))
        send_planes(axis, wires[0])
        if axis == 2:
            total = sum(jnp.where(flag, 1, 0) for flag in present)
            pl.semaphore_wait(barrier, total)
        launch(axis, *wires[0])

    for load in loads[4:]:
        load.wait()
    make_operators(s_mats, lam, coeff, left, right, l1, l2, l4, l5, d12, d0)
    for axis in range(3):
        gather_near(axis, parts, found, nbr_src, nbr_idx)

    def forward_inner(t):
        base = pl.multiple_of(512 * t, 512)
        x = jnp.concatenate([field[pl.ds(base, 256), :], field[pl.ds(base + 256, 256), :]], axis=1)
        high, low = split2(x)
        out = dot(l1[:, 0:768], jnp.concatenate([high, low, high], axis=0))
        mid[2 * t + 1] = out[:, :SLOTS]
        mid[2 * t + 2] = out[:, SLOTS:]

    @pl.loop(0, 2)
    def _(t):
        for n in range(4):
            forward_inner(4 * t + n)

    for axis in (0, 1, 2):
        await_axis(axis, *wires[0])
    for axis in (0, 1, 2):
        gather_far(axis, arrived.at[0], found, ghosts, nbr_src, nbr_idx, orient)

    high, low = split2(ghosts[0])
    out = dot(l1[:, 0:768], jnp.concatenate([high, low, high], axis=0))
    mid[0] = out[:, :SLOTS]
    mid[17] = out[:, SLOTS:]

    def forward_outer(t):
        half = aligned(32 * t, 32)
        extra = jnp.concatenate(
            [
                jnp.concatenate(
                    [
                        ghosts[axis, pl.ds(half + 16 * n, 16), SLOTS * side : SLOTS * side + SLOTS]
                        for axis in (1, 2)
                        for side in (0, 1)
                    ],
                    axis=0,
                )
                for n in (0, 1)
            ],
            axis=1,
        )
        high, low = split2(extra)
        out = dot(l1[:, 768:960], jnp.concatenate([high, low, high], axis=0))
        mid[2 * t + 1] += out[:, :SLOTS]
        mid[2 * t + 2] += out[:, SLOTS:]

    for t in range(8):
        forward_outer(t)

    def middle(g):
        start = pl.multiple_of(16 * g, 16)
        block = mid[:, pl.ds(start, 16), :]
        y = jnp.concatenate([block[:, 0:8].reshape(144, SLOTS), block[:, 8:16].reshape(144, SLOTS)], axis=1)
        high, low = split2(y)
        z = dot(l2[:, 0:432], jnp.concatenate([high, low, high], axis=0))
        d = d12[pl.ds(start, 16), :]
        d = jnp.concatenate([d[0:8], d[8:16]], axis=1)
        base = d0[...]
        base = jnp.concatenate([base, base], axis=1)
        z = z / (base + jnp.concatenate([d] * NE, axis=0))
        high, low = split2(z)
        u = dot(l4[:, 0:432], jnp.concatenate([high, low, high], axis=0))
        mid[:, pl.ds(start, 8), :] = u[:, :SLOTS].reshape(NE, 8, SLOTS)
        mid[:, pl.ds(start + 8, 8), :] = u[:, SLOTS:].reshape(NE, 8, SLOTS)

    @pl.loop(0, 3)
    def _(g):
        for n in range(7):
            middle(7 * g + n)

    def spread(first, second):
        u = jnp.concatenate([mid[first], mid[second]], axis=1)
        high, low = split2(u)
        return jnp.concatenate([high, low, high, jnp.zeros((16, 256), BF)], axis=0)

    parts[0, 0], parts[0, 1] = split2(dot(l5[0:256, :], spread(0, 17)))
    send_planes(0, wires[1])
    launch(0, *wires[1])

    def inverse(t):
        out = dot(l5[...], spread(2 * t + 1, 2 * t + 2))
        base = pl.multiple_of(512 * t, 512)
        half = aligned(32 * t, 32)
        for n in range(2):
            lanes = slice(SLOTS * n, SLOTS * n + SLOTS)
            solved[pl.ds(base + 256 * n, 256), :] = out[0:256, lanes]
            for axis in (1, 2):
                for side in (0, 1):
                    start = 256 + 32 * (axis - 1) + 16 * side
                    high, low = split2(out[start : start + 16, lanes])
                    rows = pl.ds(half + 16 * n, 16)
                    parts[axis, 0, rows, SLOTS * side : SLOTS * side + SLOTS] = high
                    parts[axis, 1, rows, SLOTS * side : SLOTS * side + SLOTS] = low

    @pl.loop(0, 2)
    def _(t):
        for n in range(4):
            inverse(4 * t + n)

    for axis in (2, 1):
        send_planes(axis, wires[1])
        launch(axis, *wires[1])
    for axis in range(3):
        gather_near(axis, parts, found, nbr_src, nbr_idx)
    for axis in (0, 1, 2):
        await_axis(axis, *wires[1])
    for axis in (0, 1, 2):
        gather_far(axis, arrived.at[1], found, ghosts, nbr_src, nbr_idx, orient)
    rank = lax.broadcasted_iota(jnp.int32, (16, 16, SLOTS), 1)

    @pl.loop(0, 8)
    def _(t):
        for n in range(2):
            half = pl.multiple_of(32 * t + 16 * n, 16)
            base = pl.multiple_of(512 * t + 256 * n, 256)
            inner = ghosts[2, pl.ds(half, 16), :]
            low = jnp.broadcast_to(inner[:, None, :SLOTS], (16, 16, SLOTS))
            high = jnp.broadcast_to(inner[:, None, SLOTS:], (16, 16, SLOTS))
            added = jnp.where(rank == 1, low, jnp.where(rank == 14, high, 0.0)).reshape(256, SLOTS)
            solved[pl.ds(base, 256), :] += added
            solved[pl.ds(base + 16, 16), :] += ghosts[1, pl.ds(half, 16), :SLOTS]
            solved[pl.ds(base + 224, 16), :] += ghosts[1, pl.ds(half, 16), SLOTS:]

    solved[256:512, :] += ghosts[0, :, :SLOTS]
    solved[14 * 256 : 15 * 256, :] += ghosts[0, :, SLOTS:]


def shards(field, s_mats, lam, coeff, nbr_src, nbr_idx, orient, send_x, send_y, send_z):
    left, right = (jnp.asarray(table, BF) for table in make_tables())
    flat = field.reshape(4096, SLOTS)
    inputs = (flat, s_mats, lam, coeff, nbr_src, nbr_idx, orient, send_x, send_y, send_z, left, right)
    out = pl.pallas_call(
        smooth_kernel,
        out_shape=jax.ShapeDtypeStruct((4096, SLOTS), F32),
        in_specs=[pl.BlockSpec(memory_space=pltpu.HBM)] * 12,
        out_specs=VMEM,
        scratch_shapes=[pltpu.VMEM(value.shape, value.dtype) for value in inputs]
        + [
            pltpu.VMEM((ROWS, 1024), BF),
            pltpu.VMEM((144, 512), BF),
            pltpu.VMEM((144, 512), BF),
            pltpu.VMEM((RIM, 1024), BF),
            pltpu.VMEM((ROWS, SLOTS), F32),
            pltpu.VMEM((144, SLOTS), F32),
            pltpu.VMEM((8, SLOTS), jnp.int32),
            pltpu.VMEM((3, 2, 256, 256), BF),
            pltpu.VMEM((3, 256, 256), F32),
            pltpu.VMEM((3, 256, 256), F32),
            pltpu.VMEM((NE, ROWS, SLOTS), F32),
            pltpu.VMEM((192, 256), F32),
            pltpu.VMEM((2, 192, 256), F32),
            pltpu.SemaphoreType.DMA((12,)),
            pltpu.SemaphoreType.DMA((2, 6)),
            pltpu.SemaphoreType.DMA((2, 6)),
        ],
        compiler_params=pltpu.CompilerParams(collective_id=0, has_side_effects=True, vmem_limit_bytes=24 << 20),
        name="smooth",
    )(*(pltpu.with_memory_space_constraint(value, pltpu.HBM) for value in inputs))
    return out.reshape(field.shape)


def solution(mesh):
    placed = (
        P(None, None, None, "dev"),
        P(),
        P(),
        P(None, "dev"),
        P(None, "dev"),
        P(None, "dev"),
        P(None, "dev"),
        P(None, "dev"),
        P(None, "dev"),
        P(None, "dev"),
    )
    return jax.shard_map(
        shards, mesh=mesh, in_specs=placed, out_specs=P(None, None, None, "dev"), check_vma=False
    )
```

```python
import functools

import jax
import jax.numpy as jnp
import numpy as np
from jax import lax
from jax.experimental import pallas as pl
from jax.experimental.pallas import tpu as pltpu
from jax.sharding import PartitionSpec as P

NP = 16
NE = 18
SLOTS = 128
ROWS = 336
RIM = 320
COUNTS = (16, 16, 64)
STARTS = (0, 32, 64)
OFFSETS = (-1, 1, -4, 4, -16, 16)
BF = jnp.bfloat16
F32 = jnp.float32
VMEM = pl.BlockSpec(memory_space=pltpu.VMEM)


def make_tables():
    b, c = np.divmod(np.arange(NE * NE), NE)
    row = np.where(c < 16, 16 * b + c, 288 + 24 * (c - 16) + b)
    inner = np.arange(1, 17)
    low, high = np.zeros(16, int), np.full(16, 17)
    jq = np.concatenate([np.repeat(inner, 16), low, high, inner, inner])
    kq = np.concatenate([np.tile(inner, 16), inner, inner, low, high])
    cols = np.concatenate([np.arange(256), np.tile(np.arange(256, 320), 3)])
    qj, qk, qi = np.zeros((3, 32, 512))
    qj[jq[cols], np.arange(448)] = 1
    qk[kq[cols], np.arange(448)] = 1
    qi[np.arange(432) % 144 // 8, np.arange(432)] = 1
    qb, qc = np.zeros((2, 32, 1024))
    for t in range(3):
        qb[b, ROWS * t + row] = 1
        qc[c, ROWS * t + row] = 1
    return np.concatenate([qj, qk, qi, qb, qc], axis=1)


def split2(x):
    high = x.astype(BF)
    return high, (x - high.astype(F32)).astype(BF)


def split3(x):
    high = x.astype(BF)
    rest = x - high.astype(F32)
    middle = rest.astype(BF)
    return high, middle, (rest - middle.astype(F32)).astype(BF)


def dot(a, b):
    return jnp.dot(a, b, preferred_element_type=F32)


def widen(small, right):
    return sum(dot(term, right) for term in split3(small))


def pick(condition):
    return jnp.where(condition, 1.0, 0.0).astype(BF)


def aligned(index, step):
    return index if isinstance(index, int) else pl.multiple_of(index, step)


def list_rows(direction):
    axis, side = direction // 2, direction % 2
    return STARTS[axis] + side * COUNTS[axis], COUNTS[axis]


def find_neighbours(me):
    spot = (lax.rem(me, 4), lax.rem(lax.div(me, 4), 4), lax.div(me, 16))
    tops = (3, 3, 15)
    return [spot[d // 2] > 0 if d % 2 == 0 else spot[d // 2] < tops[d // 2] for d in range(6)]


def greet(me, present):
    barrier = pltpu.get_barrier_semaphore()
    for direction in range(6):

        @pl.when(present[direction])
        def _():
            pl.semaphore_signal(
                barrier, inc=1, device_id=(me + OFFSETS[direction],), device_id_type=pl.DeviceIdType.MESH
            )

    return barrier


def outgoing(me, direction, msgs, arrived, send_sem, recv_sem):
    start, count = list_rows(direction)
    return pltpu.make_async_remote_copy(
        src_ref=msgs.at[pl.ds(start, count)],
        dst_ref=arrived.at[pl.ds(start, count)],
        send_sem=send_sem.at[direction],
        recv_sem=recv_sem.at[direction],
        device_id=(me + OFFSETS[direction],),
        device_id_type=pl.DeviceIdType.MESH,
    )


def send_axis(axis, me, present, parts, send, msgs, arrived, send_sem, recv_sem):
    count = 2 * COUNTS[axis]
    ids = send[axis : axis + 1, :] - 256 * axis
    chosen = pick(lax.broadcasted_iota(jnp.int32, (256, SLOTS), 0) == ids)
    found = dot(parts[axis, 0], chosen) + dot(parts[axis, 1], chosen)
    msgs[STARTS[axis] : STARTS[axis] + count, :] = found.T[:count]


def launch(axis, me, present, msgs, arrived, send_sem, recv_sem):
    for direction in (2 * axis, 2 * axis + 1):

        @pl.when(present[direction])
        def _():
            outgoing(me, direction, msgs, arrived, send_sem, recv_sem).start()


def await_axis(axis, me, present, msgs, arrived, send_sem, recv_sem):
    for direction in (2 * axis, 2 * axis + 1):

        @pl.when(present[direction])
        def _():
            outgoing(me, direction, msgs, arrived, send_sem, recv_sem).wait_send()

        @pl.when(present[direction ^ 1])
        def _():
            outgoing(me, direction, msgs, arrived, send_sem, recv_sem).wait_recv()


def pair(table, axis):
    return jnp.concatenate([table[2 * axis : 2 * axis + 1, :], table[2 * axis + 1 : 2 * axis + 2, :]], axis=1)


def gather_near(axis, parts, found, nbr_src, nbr_idx):
    src = pair(nbr_src, axis)
    idx = pair(nbr_idx, axis)
    here = jnp.where(src == 1, idx - 256 * axis, -1)
    near = pick(lax.broadcasted_iota(jnp.int32, (256, 256), 0) == here)
    found[axis] = dot(parts[axis, 0], near) + dot(parts[axis, 1], near)


def gather_far(axis, arrived, found, out, nbr_src, nbr_idx, orient):
    count = COUNTS[axis]
    src = pair(nbr_src, axis)
    idx = pair(nbr_idx, axis)
    codes = pair(orient, axis)
    there = jnp.where(src == 2 + 2 * axis, idx, jnp.where(src == 3 + 2 * axis, idx + count, -1))
    far = pick(lax.broadcasted_iota(jnp.int32, (2 * count, 256), 0) == there)
    high, low = split2(arrived[STARTS[axis] : STARTS[axis] + 2 * count, :].T)
    found[axis] += dot(high, far) + dot(low, far)
    first = codes % 2 == 1
    second = codes >= 2
    back = 7 - lax.broadcasted_iota(jnp.int32, (8, SLOTS), 0)
    for lanes in (slice(0, SLOTS), slice(SLOTS, 2 * SLOTS)):
        for u in range(16):
            rows = [
                jnp.where(
                    first[:, lanes],
                    found[axis, 16 * (15 - u) + 8 * n : 16 * (15 - u) + 8 * n + 8, lanes],
                    found[axis, 16 * u + 8 * n : 16 * u + 8 * n + 8, lanes],
                )
                for n in (0, 1)
            ]
            for n in (0, 1):
                turned = jnp.take_along_axis(rows[1 - n], back, axis=0)
                out[axis, 16 * u + 8 * n : 16 * u + 8 * n + 8, lanes] = jnp.where(second[:, lanes], turned, rows[n])


def face_planes(axis, field):
    if axis == 0:
        both = [field[256:512, :], field[14 * 256 : 15 * 256, :]]
    elif axis == 1:
        both = [
            jnp.concatenate([field[256 * i + 16 * j : 256 * i + 16 * j + 16, :] for i in range(16)], axis=0)
            for j in (1, 14)
        ]
    else:
        both = [field[pl.ds(k, 256, stride=16), :] for k in (1, 14)]
    return jnp.concatenate(both, axis=1)


def store_terms(value, out, rows, highs, lows):
    high, low = split2(value)
    for start in highs:
        out[rows, start : start + SLOTS] = high
    for start in lows:
        out[rows, start : start + SLOTS] = low


def store_mixed(value, out, rows, start, bound):
    high, low = split2(value)
    lane = lax.broadcasted_iota(jnp.int32, value.shape, 1)
    out[rows, start : start + SLOTS] = jnp.where(lane < bound, high.astype(F32), low.astype(F32)).astype(BF)


def store_tile(value, out, rows, tile, bound):
    start = SLOTS * tile
    if start + SLOTS <= bound:
        store_terms(value, out, rows, (start,), ())
    elif start >= bound:
        store_terms(value, out, rows, (), (start,))
    else:
        store_mixed(value, out, rows, start, bound - start)


def make_operators(s_mats, lam, coeff, right, l1, l2, l4, l5, l5r, d12, d0):
    room = ((0, 14), (0, 14))
    mats = [jnp.pad(s_mats[axis], room) for axis in range(3)]
    turned = [jnp.pad(s_mats[axis].T, room) for axis in range(3)]

    def tail(a, b, join):
        return jnp.concatenate([join(a[0:24], b[16:17]), join(a[0:24], b[17:18])], axis=0)

    first = widen(turned[1], right[:, 0:512])
    second = widen(turned[2], right[:, 512:1024])
    for tile in range(4):
        lanes = slice(SLOTS * tile, SLOTS * tile + SLOTS)
        a, b = first[:, lanes], second[:, lanes]
        blocks = [(slice(16 * n, 16 * n + 16), a[n : n + 1] * b[0:16]) for n in range(NE)]
        blocks.append((slice(288, 336), tail(a, b, jnp.multiply)))
        for rows, value in blocks:
            if tile < 2:
                store_terms(value, l1, rows, (SLOTS * tile, SLOTS * tile + 256), (SLOTS * tile + 512,))
            elif tile == 2:
                store_terms(value, l1, rows, (768,), ())
            else:
                store_terms(value, l1, rows, (), (896,))

    same = (lax.broadcasted_iota(jnp.int32, (8, SLOTS), 0) == (lax.broadcasted_iota(jnp.int32, (8, SLOTS), 1) & 7))
    for mat, out in ((turned[0], l2), (mats[0], l4)):
        wide = widen(mat, right[:, 1024:1536])
        for tile in range(4):
            part = wide[:, SLOTS * tile : SLOTS * tile + SLOTS]
            for n in range(0, NE, 2):
                value = jnp.concatenate([jnp.where(same, part[m : m + 1], 0.0) for m in (n, n + 1)], axis=0)
                store_tile(value, out, slice(8 * n, 8 * n + 16), tile, 288)

    first = widen(pltpu.roll(mats[1], 31, 0), right[:, 1536:2560])
    second = widen(pltpu.roll(mats[2], 31, 0), right[:, 2560:3584])
    for tile in range(8):
        lanes = slice(SLOTS * tile, SLOTS * tile + SLOTS)
        a, b = first[:, lanes], second[:, lanes]
        values = [a[n : n + 1] * b[0:16] for n in (*range(16), 31, 16)]
        values += [a[0:16] * b[n : n + 1] for n in (31, 16)]
        for n, value in enumerate(values[:16]):
            store_tile(value, l5, slice(16 * n, 16 * n + 16), tile, 2 * ROWS)
        for n, value in enumerate(values[16:] if tile < 3 else ()):
            high, low = split2(value)
            l5r[16 * n : 16 * n + 16, lanes] = high
            l5r[64 + 16 * n : 64 + 16 * n + 16, lanes] = low

    levels = jnp.pad(lam[...], ((0, 5), (0, 110))).T[:32]
    products = [levels[:, axis : axis + 1] * coeff[axis : axis + 1, :] for axis in range(3)]
    for n in range(NE):
        d12[16 * n : 16 * n + 16, :] = products[1][n : n + 1] + products[2][0:16]
        d0[8 * n : 8 * n + 8, :] = jnp.broadcast_to(products[0][n : n + 1], (8, SLOTS))
    d12[288:336, :] = tail(products[1], products[2], jnp.add)


def smooth_kernel(
    field_in, s_mats_in, lam_in, coeff_in, src_in, idx_in, orient_in, send_x_in, send_y_in, send_z_in, right_in,
    solved,
    field, s_mats, lam, coeff, nbr_src, nbr_idx, orient, send_x, send_y, send_z, right,
    l1, l2, l4, l5, l5r, d12, d0, send, parts, found, ghosts, mid, u_high, u_low,
    msgs, arrived, load_sem, send_sem, recv_sem,
):
    me = lax.axis_index("dev")
    loads = [
        pltpu.make_async_copy(source, target, load_sem.at[n])
        for n, (source, target) in enumerate(
            (
                (send_x_in, send_x), (send_y_in, send_y), (send_z_in, send_z), (field_in, field),
                (s_mats_in, s_mats), (right_in, right), (lam_in, lam), (coeff_in, coeff),
                (src_in, nbr_src), (idx_in, nbr_idx), (orient_in, orient),
            )
        )
    ]
    for load in loads:
        load.start()
    present = find_neighbours(me)
    for direction in range(6):
        start, count = list_rows(direction)

        @pl.when(jnp.logical_not(present[direction ^ 1]))
        def _():
            for phase in range(2):
                arrived[phase, start : start + count, :] = jnp.zeros((count, 256), F32)

    barrier = greet(me, present)
    for load in loads[:4]:
        load.wait()
    send[...] = jnp.full((8, SLOTS), -1, jnp.int32)
    send[0:1, 0:16] = send_x[0:1, :]
    send[0:1, 16:32] = send_x[1:2, :]
    send[1:2, 0:16] = send_y[0:1, :]
    send[1:2, 16:32] = send_y[1:2, :]
    send[2:3, 0:64] = send_z[0:1, :]
    send[2:3, 64:128] = send_z[1:2, :]

    wires = [(me, present, msgs, arrived.at[n], send_sem.at[n], recv_sem.at[n]) for n in range(2)]

    def send_planes(axis, wire):
        send_axis(axis, *wire[:2], parts, send, *wire[2:])

    for axis in (1, 2, 0):
        parts[axis, 0], parts[axis, 1] = split2(face_planes(axis, field))
        send_planes(axis, wires[0])
    pl.semaphore_wait(barrier, sum(jnp.where(flag, 1, 0) for flag in present))
    for axis in (1, 2, 0):
        launch(axis, *wires[0])
    for load in loads[4:]:
        load.wait()
    make_operators(s_mats, lam, coeff, right, l1, l2, l4, l5, l5r, d12, d0)
    for axis in range(3):
        gather_near(axis, parts, found, nbr_src, nbr_idx)

    def forward_inner(t):
        base = pl.multiple_of(512 * t, 512)
        x = jnp.concatenate([field[pl.ds(base, 256), :], field[pl.ds(base + 256, 256), :]], axis=1)
        high, low = split2(x)
        out = dot(l1[:, 0:768], jnp.concatenate([high, low, high], axis=0))
        mid[2 * t + 1] = out[:, :SLOTS]
        mid[2 * t + 2] = out[:, SLOTS:]

    @pl.loop(0, 2)
    def _(t):
        for n in range(4):
            forward_inner(4 * t + n)

    for axis in (0, 1, 2):
        await_axis(axis, *wires[0])
    for axis in (0, 1, 2):
        gather_far(axis, arrived.at[0], found, ghosts, nbr_src, nbr_idx, orient)

    high, low = split2(ghosts[0])
    out = dot(l1[:, 0:768], jnp.concatenate([high, low, high], axis=0))
    mid[0] = out[:, :SLOTS]
    mid[17] = out[:, SLOTS:]

    def forward_outer(t):
        half = aligned(32 * t, 32)
        extra = jnp.concatenate(
            [
                jnp.concatenate(
                    [
                        ghosts[axis, pl.ds(half + 16 * n, 16), SLOTS * side : SLOTS * side + SLOTS]
                        for axis in (1, 2)
                        for side in (0, 1)
                    ],
                    axis=0,
                )
                for n in (0, 1)
            ],
            axis=1,
        )
        high, low = split2(extra)
        out = dot(l1[:, 768:960], jnp.concatenate([high, low, high], axis=0))
        mid[2 * t + 1] += out[:, :SLOTS]
        mid[2 * t + 2] += out[:, SLOTS:]

    for t in range(8):
        forward_outer(t)

    def middle(g):
        start = pl.multiple_of(16 * g, 16)
        block = mid[:, pl.ds(start, 16), :]
        y = jnp.concatenate([block[:, 0:8].reshape(144, SLOTS), block[:, 8:16].reshape(144, SLOTS)], axis=1)
        high, low = split2(y)
        z = dot(l2[:, 0:432], jnp.concatenate([high, low, high], axis=0))
        d = d12[pl.ds(start, 16), :]
        d = jnp.concatenate([d[0:8], d[8:16]], axis=1)
        base = d0[...]
        base = jnp.concatenate([base, base], axis=1)
        z = z / (base + jnp.concatenate([d] * NE, axis=0))
        high, low = split2(z)
        u = dot(l4[:, 0:432], jnp.concatenate([high, low, high], axis=0))
        high, low = split2(
            jnp.concatenate([u[:, :SLOTS].reshape(NE, 8, SLOTS), u[:, SLOTS:].reshape(NE, 8, SLOTS)], axis=1)
        )
        u_high[:, pl.ds(start, 16), :] = high
        u_low[:, pl.ds(start, 16), :] = low

    @pl.loop(0, 3)
    def _(g):
        for n in range(7):
            middle(7 * g + n)

    def spread(first, second):
        high = jnp.concatenate([u_high[first], u_high[second]], axis=1)
        low = jnp.concatenate([u_low[first], u_low[second]], axis=1)
        return high, low

    def inverse(first, second):
        high, low = spread(first, second)
        return dot(l5[...], jnp.concatenate([high, low, high, jnp.zeros((16, 256), BF)], axis=0))

    for t in range(8):
        high, low = spread(2 * t + 1, 2 * t + 2)
        both = dot(l5r[:, 0:ROWS], high)
        out = both[0:64] + both[64:128] + dot(l5r[0:64, 0:ROWS], low)
        for axis in (1, 2):
            for side in (0, 1):
                start = 32 * (axis - 1) + 16 * side
                rows = slice(32 * t, 32 * t + 32)
                lanes = slice(SLOTS * side, SLOTS * side + SLOTS)
                block = out[start : start + 16]
                block = jnp.concatenate([block[:, :SLOTS], block[:, SLOTS:]], axis=0)
                parts[axis, 0, rows, lanes], parts[axis, 1, rows, lanes] = split2(block)
    parts[0, 0], parts[0, 1] = split2(inverse(0, 17))
    for axis in (1, 2, 0):
        send_planes(axis, wires[1])
    for axis in (1, 2, 0):
        launch(axis, *wires[1])
    for t in range(8):
        out = inverse(2 * t + 1, 2 * t + 2)
        solved[512 * t : 512 * t + 256, :] = out[:, :SLOTS]
        solved[512 * t + 256 : 512 * t + 512, :] = out[:, SLOTS:]
    for axis in range(3):
        gather_near(axis, parts, found, nbr_src, nbr_idx)
    for axis in (0, 1, 2):
        await_axis(axis, *wires[1])
    for axis in (0, 1, 2):
        gather_far(axis, arrived.at[1], found, ghosts, nbr_src, nbr_idx, orient)
    rank = lax.broadcasted_iota(jnp.int32, (16, 16, SLOTS), 1)

    @pl.loop(0, 8)
    def _(t):
        for n in range(2):
            half = pl.multiple_of(32 * t + 16 * n, 16)
            base = pl.multiple_of(512 * t + 256 * n, 256)
            inner = ghosts[2, pl.ds(half, 16), :]
            low = jnp.broadcast_to(inner[:, None, :SLOTS], (16, 16, SLOTS))
            high = jnp.broadcast_to(inner[:, None, SLOTS:], (16, 16, SLOTS))
            added = jnp.where(rank == 1, low, jnp.where(rank == 14, high, 0.0)).reshape(256, SLOTS)
            solved[pl.ds(base, 256), :] += added
            solved[pl.ds(base + 16, 16), :] += ghosts[1, pl.ds(half, 16), :SLOTS]
            solved[pl.ds(base + 224, 16), :] += ghosts[1, pl.ds(half, 16), SLOTS:]

    solved[256:512, :] += ghosts[0, :, :SLOTS]
    solved[14 * 256 : 15 * 256, :] += ghosts[0, :, SLOTS:]


def shards(field, s_mats, lam, coeff, nbr_src, nbr_idx, orient, send_x, send_y, send_z):
    right = jnp.asarray(make_tables(), BF)
    flat = field.reshape(4096, SLOTS)
    inputs = (flat, s_mats, lam, coeff, nbr_src, nbr_idx, orient, send_x, send_y, send_z, right)
    out = pl.pallas_call(
        smooth_kernel,
        out_shape=jax.ShapeDtypeStruct((4096, SLOTS), F32),
        in_specs=[pl.BlockSpec(memory_space=pltpu.HBM)] * 11,
        out_specs=VMEM,
        scratch_shapes=[pltpu.VMEM(value.shape, value.dtype) for value in inputs]
        + [
            pltpu.VMEM((ROWS, 1024), BF),
            pltpu.VMEM((144, 512), BF),
            pltpu.VMEM((144, 512), BF),
            pltpu.VMEM((256, 1024), BF),
            pltpu.VMEM((128, 384), BF),
            pltpu.VMEM((ROWS, SLOTS), F32),
            pltpu.VMEM((144, SLOTS), F32),
            pltpu.VMEM((8, SLOTS), jnp.int32),
            pltpu.VMEM((3, 2, 256, 256), BF),
            pltpu.VMEM((3, 256, 256), F32),
            pltpu.VMEM((3, 256, 256), F32),
            pltpu.VMEM((NE, ROWS, SLOTS), F32),
            pltpu.VMEM((NE, ROWS, SLOTS), BF),
            pltpu.VMEM((NE, ROWS, SLOTS), BF),
            pltpu.VMEM((192, 256), F32),
            pltpu.VMEM((2, 192, 256), F32),
            pltpu.SemaphoreType.DMA((11,)),
            pltpu.SemaphoreType.DMA((2, 6)),
            pltpu.SemaphoreType.DMA((2, 6)),
        ],
        compiler_params=pltpu.CompilerParams(collective_id=0, has_side_effects=True, vmem_limit_bytes=24 << 20),
        name="smooth",
    )(*(pltpu.with_memory_space_constraint(value, pltpu.HBM) for value in inputs))
    return out.reshape(field.shape)


def solution(mesh):
    placed = (
        P(None, None, None, "dev"),
        P(),
        P(),
        P(None, "dev"),
        P(None, "dev"),
        P(None, "dev"),
        P(None, "dev"),
        P(None, "dev"),
        P(None, "dev"),
        P(None, "dev"),
    )
    return jax.shard_map(
        shards, mesh=mesh, in_specs=placed, out_specs=P(None, None, None, "dev"), check_vma=False
    )
```

```python
import functools

import jax
import jax.numpy as jnp
import numpy as np
from jax import lax
from jax.experimental import pallas as pl
from jax.experimental.pallas import tpu as pltpu
from jax.sharding import PartitionSpec as P

NP = 16
NE = 18
SLOTS = 128
ROWS = 336
RIM = 320
COUNTS = (16, 16, 64)
STARTS = (0, 32, 64)
OFFSETS = (-1, 1, -4, 4, -16, 16)
BF = jnp.bfloat16
F32 = jnp.float32
VMEM = pl.BlockSpec(memory_space=pltpu.VMEM)


def make_tables():
    b, c = np.divmod(np.arange(NE * NE), NE)
    row = np.where(c < 16, 16 * b + c, 288 + 24 * (c - 16) + b)
    inner = np.arange(1, 17)
    low, high = np.zeros(16, int), np.full(16, 17)
    jq = np.concatenate([np.repeat(inner, 16), low, high, inner, inner])
    kq = np.concatenate([np.tile(inner, 16), inner, inner, low, high])
    cols = np.concatenate([np.arange(256), np.tile(np.arange(256, 320), 3)])
    qj, qk, qi = np.zeros((3, 32, 512))
    qe = np.zeros((32, SLOTS))
    qj[jq[cols], np.arange(448)] = 1
    qk[kq[cols], np.arange(448)] = 1
    qi[np.arange(432) % 144 // 8, np.arange(432)] = 1
    qe[1 + np.arange(128) // 8, np.arange(128)] = 1
    qb, qc = np.zeros((2, 32, 1024))
    for t in range(3):
        qb[b, ROWS * t + row] = 1
        qc[c, ROWS * t + row] = 1
    return np.concatenate([qj, qk, qi, qb, qc, qe], axis=1)


def split2(x):
    high = x.astype(BF)
    return high, (x - high.astype(F32)).astype(BF)


def split3(x):
    high = x.astype(BF)
    rest = x - high.astype(F32)
    middle = rest.astype(BF)
    return high, middle, (rest - middle.astype(F32)).astype(BF)


def dot(a, b):
    return jnp.dot(a, b, preferred_element_type=F32)


def widen(small, right):
    return sum(dot(term, right) for term in split3(small))


def pick(condition):
    return jnp.where(condition, 1.0, 0.0).astype(BF)


def aligned(index, step):
    return index if isinstance(index, int) else pl.multiple_of(index, step)


def face_index(face):
    return (slice(None),) * (face // 2) + (14 if face % 2 else 1,)


def list_rows(direction):
    axis, side = direction // 2, direction % 2
    return STARTS[axis] + side * COUNTS[axis], COUNTS[axis]


def find_neighbours(me):
    spot = (lax.rem(me, 4), lax.rem(lax.div(me, 4), 4), lax.div(me, 16))
    tops = (3, 3, 15)
    return [spot[d // 2] > 0 if d % 2 == 0 else spot[d // 2] < tops[d // 2] for d in range(6)]


def greet(me, present):
    barrier = pltpu.get_barrier_semaphore()
    for direction in range(6):

        @pl.when(present[direction])
        def _():
            pl.semaphore_signal(
                barrier, inc=1, device_id=(me + OFFSETS[direction],), device_id_type=pl.DeviceIdType.MESH
            )

    return barrier


def outgoing(me, direction, msgs, arrived, send_sem, recv_sem):
    start, count = list_rows(direction)
    return pltpu.make_async_remote_copy(
        src_ref=msgs.at[pl.ds(start, count)],
        dst_ref=arrived.at[pl.ds(start, count)],
        send_sem=send_sem.at[direction],
        recv_sem=recv_sem.at[direction],
        device_id=(me + OFFSETS[direction],),
        device_id_type=pl.DeviceIdType.MESH,
    )


def send_axis(axis, me, present, parts, send, msgs, arrived, send_sem, recv_sem):
    count = 2 * COUNTS[axis]
    ids = send[axis : axis + 1, :] - 256 * axis
    chosen = pick(lax.broadcasted_iota(jnp.int32, (256, SLOTS), 0) == ids)
    found = dot(parts[axis, 0], chosen) + dot(parts[axis, 1], chosen)
    msgs[STARTS[axis] : STARTS[axis] + count, :] = found.T[:count]


def launch(axis, me, present, msgs, arrived, send_sem, recv_sem):
    for direction in (2 * axis, 2 * axis + 1):

        @pl.when(present[direction])
        def _():
            outgoing(me, direction, msgs, arrived, send_sem, recv_sem).start()


def await_axis(axis, me, present, msgs, arrived, send_sem, recv_sem):
    for direction in (2 * axis, 2 * axis + 1):

        @pl.when(present[direction])
        def _():
            outgoing(me, direction, msgs, arrived, send_sem, recv_sem).wait_send()

        @pl.when(present[direction ^ 1])
        def _():
            outgoing(me, direction, msgs, arrived, send_sem, recv_sem).wait_recv()


def pair(table, axis):
    return jnp.concatenate([table[2 * axis : 2 * axis + 1, :], table[2 * axis + 1 : 2 * axis + 2, :]], axis=1)


def gather_near(axis, parts, found, nbr_src, nbr_idx):
    src = pair(nbr_src, axis)
    idx = pair(nbr_idx, axis)
    here = jnp.where(src == 1, idx - 256 * axis, -1)
    near = pick(lax.broadcasted_iota(jnp.int32, (256, 256), 0) == here)
    found[axis] = dot(parts[axis, 0], near) + dot(parts[axis, 1], near)


def gather_far(axis, arrived, found, out, nbr_src, nbr_idx, orient):
    count = COUNTS[axis]
    src = pair(nbr_src, axis)
    idx = pair(nbr_idx, axis)
    codes = pair(orient, axis)
    there = jnp.where(src == 2 + 2 * axis, idx, jnp.where(src == 3 + 2 * axis, idx + count, -1))
    far = pick(lax.broadcasted_iota(jnp.int32, (2 * count, 256), 0) == there)
    high, low = split2(arrived[STARTS[axis] : STARTS[axis] + 2 * count, :].T)
    found[axis] += dot(high, far) + dot(low, far)
    first = codes % 2 == 1
    second = codes >= 2
    back = 7 - lax.broadcasted_iota(jnp.int32, (8, SLOTS), 0)
    for lanes in (slice(0, SLOTS), slice(SLOTS, 2 * SLOTS)):
        for u in range(16):
            rows = [
                jnp.where(
                    first[:, lanes],
                    found[axis, 16 * (15 - u) + 8 * n : 16 * (15 - u) + 8 * n + 8, lanes],
                    found[axis, 16 * u + 8 * n : 16 * u + 8 * n + 8, lanes],
                )
                for n in (0, 1)
            ]
            for n in (0, 1):
                turned = jnp.take_along_axis(rows[1 - n], back, axis=0)
                out[axis, 16 * u + 8 * n : 16 * u + 8 * n + 8, lanes] = jnp.where(second[:, lanes], turned, rows[n])


def store_terms(value, out, rows, highs, lows):
    high, low = split2(value)
    for start in highs:
        out[rows, start : start + SLOTS] = high
    for start in lows:
        out[rows, start : start + SLOTS] = low


def store_mixed(value, out, rows, start, bound):
    high, low = split2(value)
    lane = lax.broadcasted_iota(jnp.int32, value.shape, 1)
    out[rows, start : start + SLOTS] = jnp.where(lane < bound, high.astype(F32), low.astype(F32)).astype(BF)


def store_tile(value, out, rows, tile, bound):
    start = SLOTS * tile
    if start + SLOTS <= bound:
        store_terms(value, out, rows, (start,), ())
    elif start >= bound:
        store_terms(value, out, rows, (), (start,))
    else:
        store_mixed(value, out, rows, start, bound - start)


def make_operators(s_mats, lam, coeff, right, l1, l2, l4, l5, l5r, d12, d0, factors):
    room = ((0, 14), (0, 14))
    mats = [jnp.pad(s_mats[axis], room) for axis in range(3)]
    turned = [jnp.pad(s_mats[axis].T, room) for axis in range(3)]

    def tail(a, b, join):
        return jnp.concatenate([join(a[0:24], b[16:17]), join(a[0:24], b[17:18])], axis=0)

    first = widen(turned[1], right[:, 0:512])
    second = widen(turned[2], right[:, 512:1024])
    for tile in range(4):
        lanes = slice(SLOTS * tile, SLOTS * tile + SLOTS)
        a, b = first[:, lanes], second[:, lanes]
        blocks = [(slice(16 * n, 16 * n + 16), a[n : n + 1] * b[0:16]) for n in range(NE)]
        blocks.append((slice(288, 336), tail(a, b, jnp.multiply)))
        for rows, value in blocks:
            if tile < 2:
                store_terms(value, l1, rows, (SLOTS * tile, SLOTS * tile + 256), (SLOTS * tile + 512,))
            elif tile == 2:
                store_terms(value, l1, rows, (768,), ())
            else:
                store_terms(value, l1, rows, (), (896,))

    same = (lax.broadcasted_iota(jnp.int32, (8, SLOTS), 0) == (lax.broadcasted_iota(jnp.int32, (8, SLOTS), 1) & 7))
    wide = widen(turned[0], right[:, 3584:3712])
    for n in range(0, NE, 2):
        rows = slice(8 * n, 8 * n + 16)
        value = jnp.concatenate([jnp.where(same, wide[m : m + 1, :SLOTS], 0.0) for m in (n, n + 1)], axis=0)
        store_terms(value, l2, rows, (0, 128), (256,))
    wide = widen(mats[0], right[:, 1024:1536])
    for tile in range(4):
        part = wide[:, SLOTS * tile : SLOTS * tile + SLOTS]
        for n in range(0, NE, 2):
            value = jnp.concatenate([jnp.where(same, part[m : m + 1], 0.0) for m in (n, n + 1)], axis=0)
            store_tile(value, l4, slice(8 * n, 8 * n + 16), tile, 288)

    first = widen(pltpu.roll(mats[1], 31, 0), right[:, 1536:2560])
    second = widen(pltpu.roll(mats[2], 31, 0), right[:, 2560:3584])
    for tile in range(8):
        lanes = slice(SLOTS * tile, SLOTS * tile + SLOTS)
        a, b = first[:, lanes], second[:, lanes]
        values = [a[n : n + 1] * b[0:16] for n in (*range(16), 31, 16)]
        values += [a[0:16] * b[n : n + 1] for n in (31, 16)]
        for n, value in enumerate(values[:16]):
            store_tile(value, l5, slice(16 * n, 16 * n + 16), tile, 2 * ROWS)
        for n, value in enumerate(values[16:] if tile < 3 else ()):
            high, low = split2(value)
            l5r[16 * n : 16 * n + 16, lanes] = high
            l5r[64 + 16 * n : 64 + 16 * n + 16, lanes] = low

    levels = jnp.pad(lam[...], ((0, 5), (0, 110))).T[:32]
    products = [levels[:, axis : axis + 1] * coeff[axis : axis + 1, :] for axis in range(3)]
    for n in range(NE):
        d12[16 * n : 16 * n + 16, :] = products[1][n : n + 1] + products[2][0:16]
        d0[8 * n : 8 * n + 8, :] = jnp.broadcast_to(products[0][n : n + 1], (8, SLOTS))
    sides = [jnp.broadcast_to(turned[0][:, n : n + 1], (32, SLOTS)) for n in (0, 17)]
    for n in range(NE):
        for m in (0, 1):
            factors[m, 8 * n : 8 * n + 8, :] = jnp.broadcast_to(sides[m][n : n + 1], (8, SLOTS))
    d12[288:336, :] = tail(products[1], products[2], jnp.add)


def smooth_kernel(
    field_in, s_mats_in, lam_in, coeff_in, src_in, idx_in, orient_in, send_x_in, send_y_in, send_z_in, right_in,
    solved,
    field, s_mats, lam, coeff, nbr_src, nbr_idx, orient, send_x, send_y, send_z, right,
    planes, l1, l2, l4, l5, l5r, d12, d0, factors, send, parts, found, ghosts, mid, coef, edges, shells, u_high, u_low,
    msgs, arrived, load_sem, send_sem, recv_sem,
):
    me = lax.axis_index("dev")
    loads = [
        pltpu.make_async_copy(source, target, load_sem.at[n])
        for n, (source, target) in enumerate(
            (
                (send_x_in, send_x), (send_y_in, send_y), (send_z_in, send_z),
                *((field_in.at[face_index(face)], planes.at[face]) for face in (2, 3, 4, 5, 0, 1)), (field_in, field),
                (s_mats_in, s_mats), (right_in, right), (lam_in, lam), (coeff_in, coeff),
                (src_in, nbr_src), (idx_in, nbr_idx), (orient_in, orient),
            )
        )
    ]
    for load in loads:
        load.start()
    present = find_neighbours(me)
    for direction in range(6):
        start, count = list_rows(direction)

        @pl.when(jnp.logical_not(present[direction ^ 1]))
        def _():
            for phase in range(2):
                arrived[phase, start : start + count, :] = jnp.zeros((count, 256), F32)

    barrier = greet(me, present)
    for load in loads[:9]:
        load.wait()
    send[...] = jnp.full((8, SLOTS), -1, jnp.int32)
    send[0:1, 0:16] = send_x[0:1, :]
    send[0:1, 16:32] = send_x[1:2, :]
    send[1:2, 0:16] = send_y[0:1, :]
    send[1:2, 16:32] = send_y[1:2, :]
    send[2:3, 0:64] = send_z[0:1, :]
    send[2:3, 64:128] = send_z[1:2, :]

    wires = [(me, present, msgs, arrived.at[n], send_sem.at[n], recv_sem.at[n]) for n in range(2)]

    def send_planes(axis, wire):
        send_axis(axis, *wire[:2], parts, send, *wire[2:])

    for axis in (2, 1, 0):
        parts[axis, 0], parts[axis, 1] = split2(
            jnp.concatenate([planes[2 * axis + n].reshape(256, SLOTS) for n in (0, 1)], axis=1)
        )
        send_planes(axis, wires[0])
    pl.semaphore_wait(barrier, sum(jnp.where(flag, 1, 0) for flag in present))
    for axis in (2, 1, 0):
        launch(axis, *wires[0])
    for load in loads[9:]:
        load.wait()
    make_operators(s_mats, lam, coeff, right, l1, l2, l4, l5, l5r, d12, d0, factors)
    for axis in range(3):
        gather_near(axis, parts, found, nbr_src, nbr_idx)

    def forward_inner(t):
        x = jnp.concatenate([field[2 * t + n].reshape(256, SLOTS) for n in (0, 1)], axis=1)
        high, low = split2(x)
        out = dot(l1[:, 0:768], jnp.concatenate([high, low, high], axis=0))
        mid[2 * t + 1] = out[:, :SLOTS]
        mid[2 * t + 2] = out[:, SLOTS:]

    @pl.loop(0, 2)
    def _(t):
        for n in range(4):
            forward_inner(4 * t + n)

    @pl.loop(0, 3)
    def _(g):
        for n in range(7):
            start = pl.multiple_of(112 * g + 16 * n, 16)
            block = mid[1:17, pl.ds(start, 16), :]
            y = jnp.concatenate([block[:, 0:8].reshape(SLOTS, SLOTS), block[:, 8:16].reshape(SLOTS, SLOTS)], axis=1)
            high, low = split2(y)
            z = dot(l2[:, 0:384], jnp.concatenate([high, low, high], axis=0))
            coef[:, pl.ds(start, 8), :] = z[:, :SLOTS].reshape(NE, 8, SLOTS)
            coef[:, pl.ds(start + 8, 8), :] = z[:, SLOTS:].reshape(NE, 8, SLOTS)

    for axis in (0, 1, 2):
        await_axis(axis, *wires[0])
    for axis in (0, 1, 2):
        gather_far(axis, arrived.at[0], found, ghosts, nbr_src, nbr_idx, orient)

    turned = []
    for axis in (1, 2):
        for half in range(2):
            x = ghosts[axis].reshape(16, 16, 256)[:, 8 * half : 8 * half + 8, :].reshape(SLOTS, 256)
            high, low = split2(x)
            turned.append(dot(l2[:, 0:384], jnp.concatenate([high, low, high], axis=0)))
    high, low = split2(ghosts[0])
    out = dot(l1[:, 0:768], jnp.concatenate([high, low, high], axis=0))
    edges[0] = out[:, :SLOTS]
    edges[1] = out[:, SLOTS:]
    for a in range(0, NE, 2):
        extra = jnp.concatenate(
            [
                jnp.concatenate(
                    [
                        turned[2 * axis + half][8 * n : 8 * n + 8, SLOTS * side : SLOTS * side + SLOTS]
                        for axis in (0, 1)
                        for side in (0, 1)
                        for half in (0, 1)
                    ],
                    axis=0,
                )
                for n in (a, a + 1)
            ],
            axis=1,
        )
        high, low = split2(extra)
        out = dot(l1[:, 768:960], jnp.concatenate([high, low, high], axis=0))
        coef[a] += out[:, :SLOTS]
        coef[a + 1] += out[:, SLOTS:]
    for a in range(0, NE, 2):
        scaled = []
        for n in (a, a + 1):
            rows = slice(8 * n, 8 * n + 8)
            z = coef[n].reshape(42, 8, SLOTS)
            for m in (0, 1):
                z = z + factors[m, rows, :] * edges[m].reshape(42, 8, SLOTS)
            z = (z / (d0[rows, :] + d12[...].reshape(42, 8, SLOTS))).reshape(ROWS, SLOTS)
            coef[n] = z
            scaled.append(z)
        high, low = split2(jnp.concatenate(scaled, axis=1))
        both = dot(l5r[:, 0:ROWS], high)
        out = both[0:64] + both[64:128] + dot(l5r[0:64, 0:ROWS], low)
        shells[a] = out[:, :SLOTS]
        shells[a + 1] = out[:, SLOTS:]
    for axis in (2, 1):
        turned = []
        for half in range(2):
            starts = [32 * (axis - 1) + 16 * side + 8 * half for side in (0, 1)]
            x = jnp.concatenate([shells[:, start : start + 8, :].reshape(144, SLOTS) for start in starts], axis=1)
            high, low = split2(x)
            turned.append(dot(l4[:, 0:432], jnp.concatenate([high, low, high], axis=0)))
        rim = jnp.concatenate([turned[half][8 * i : 8 * i + 8] for i in range(1, 17) for half in range(2)], axis=0)
        parts[axis, 0], parts[axis, 1] = split2(rim)
    for axis in (2, 1):
        send_planes(axis, wires[1])
    for axis in (2, 1):
        launch(axis, *wires[1])
    def middle(g):
        start = pl.multiple_of(16 * g, 16)
        block = coef[:, pl.ds(start, 16), :]
        z = jnp.concatenate([block[:, 0:8].reshape(144, SLOTS), block[:, 8:16].reshape(144, SLOTS)], axis=1)
        high, low = split2(z)
        u = dot(l4[:, 0:432], jnp.concatenate([high, low, high], axis=0))
        high, low = split2(
            jnp.concatenate([u[:, :SLOTS].reshape(NE, 8, SLOTS), u[:, SLOTS:].reshape(NE, 8, SLOTS)], axis=1)
        )
        u_high[:, pl.ds(start, 16), :] = high
        u_low[:, pl.ds(start, 16), :] = low

    @pl.loop(0, 3)
    def _(g):
        for n in range(7):
            middle(7 * g + n)

    def inverse(first, second):
        high = jnp.concatenate([u_high[first], u_high[second]], axis=1)
        low = jnp.concatenate([u_low[first], u_low[second]], axis=1)
        return dot(l5[...], jnp.concatenate([high, low, high, jnp.zeros((16, 256), BF)], axis=0))

    parts[0, 0], parts[0, 1] = split2(inverse(0, 17))
    send_planes(0, wires[1])
    launch(0, *wires[1])
    for t in range(8):
        out = inverse(2 * t + 1, 2 * t + 2)
        solved[512 * t : 512 * t + 256, :] = out[:, :SLOTS]
        solved[512 * t + 256 : 512 * t + 512, :] = out[:, SLOTS:]
    for axis in range(3):
        gather_near(axis, parts, found, nbr_src, nbr_idx)
    for axis in (0, 1, 2):
        await_axis(axis, *wires[1])
    for axis in (0, 1, 2):
        gather_far(axis, arrived.at[1], found, ghosts, nbr_src, nbr_idx, orient)
    rank = lax.broadcasted_iota(jnp.int32, (16, 16, SLOTS), 1)

    @pl.loop(0, 8)
    def _(t):
        for n in range(2):
            half = pl.multiple_of(32 * t + 16 * n, 16)
            base = pl.multiple_of(512 * t + 256 * n, 256)
            inner = ghosts[2, pl.ds(half, 16), :]
            low = jnp.broadcast_to(inner[:, None, :SLOTS], (16, 16, SLOTS))
            high = jnp.broadcast_to(inner[:, None, SLOTS:], (16, 16, SLOTS))
            added = jnp.where(rank == 1, low, jnp.where(rank == 14, high, 0.0)).reshape(256, SLOTS)
            solved[pl.ds(base, 256), :] += added
            solved[pl.ds(base + 16, 16), :] += ghosts[1, pl.ds(half, 16), :SLOTS]
            solved[pl.ds(base + 224, 16), :] += ghosts[1, pl.ds(half, 16), SLOTS:]

    solved[256:512, :] += ghosts[0, :, :SLOTS]
    solved[14 * 256 : 15 * 256, :] += ghosts[0, :, SLOTS:]


def shards(field, s_mats, lam, coeff, nbr_src, nbr_idx, orient, send_x, send_y, send_z):
    right = jnp.asarray(make_tables(), BF)
    inputs = (field, s_mats, lam, coeff, nbr_src, nbr_idx, orient, send_x, send_y, send_z, right)
    out = pl.pallas_call(
        smooth_kernel,
        out_shape=jax.ShapeDtypeStruct((4096, SLOTS), F32),
        in_specs=[pl.BlockSpec(memory_space=pltpu.HBM)] * 11,
        out_specs=VMEM,
        scratch_shapes=[pltpu.VMEM(value.shape, value.dtype) for value in inputs]
        + [
            pltpu.VMEM((6, 16, 16, SLOTS), F32),
            pltpu.VMEM((ROWS, 1024), BF),
            pltpu.VMEM((144, 384), BF),
            pltpu.VMEM((144, 512), BF),
            pltpu.VMEM((256, 1024), BF),
            pltpu.VMEM((128, 384), BF),
            pltpu.VMEM((ROWS, SLOTS), F32),
            pltpu.VMEM((144, SLOTS), F32),
            pltpu.VMEM((2, 144, SLOTS), F32),
            pltpu.VMEM((8, SLOTS), jnp.int32),
            pltpu.VMEM((3, 2, 256, 256), BF),
            pltpu.VMEM((3, 256, 256), F32),
            pltpu.VMEM((3, 256, 256), F32),
            pltpu.VMEM((NE, ROWS, SLOTS), F32),
            pltpu.VMEM((NE, ROWS, SLOTS), F32),
            pltpu.VMEM((2, ROWS, SLOTS), F32),
            pltpu.VMEM((NE, 64, SLOTS), F32),
            pltpu.VMEM((NE, ROWS, SLOTS), BF),
            pltpu.VMEM((NE, ROWS, SLOTS), BF),
            pltpu.VMEM((192, 256), F32),
            pltpu.VMEM((2, 192, 256), F32),
            pltpu.SemaphoreType.DMA((17,)),
            pltpu.SemaphoreType.DMA((2, 6)),
            pltpu.SemaphoreType.DMA((2, 6)),
        ],
        compiler_params=pltpu.CompilerParams(collective_id=0, has_side_effects=True, vmem_limit_bytes=24 << 20),
        name="smooth",
    )(*(pltpu.with_memory_space_constraint(value, pltpu.HBM) for value in inputs))
    return out.reshape(field.shape)


def solution(mesh):
    placed = (
        P(None, None, None, "dev"),
        P(),
        P(),
        P(None, "dev"),
        P(None, "dev"),
        P(None, "dev"),
        P(None, "dev"),
        P(None, "dev"),
        P(None, "dev"),
        P(None, "dev"),
    )
    return jax.shard_map(
        shards, mesh=mesh, in_specs=placed, out_specs=P(None, None, None, "dev"), check_vma=False
    )
```

```python
import functools

import jax
import jax.numpy as jnp
import numpy as np
from jax import lax
from jax.experimental import pallas as pl
from jax.experimental.pallas import tpu as pltpu
from jax.sharding import PartitionSpec as P

NP = 16
NE = 18
SLOTS = 128
ROWS = 336
RIM = 320
COUNTS = (16, 16, 64)
STARTS = (0, 32, 64)
OFFSETS = (-1, 1, -4, 4, -16, 16)
BF = jnp.bfloat16
F32 = jnp.float32
VMEM = pl.BlockSpec(memory_space=pltpu.VMEM)


def make_tables():
    b, c = np.divmod(np.arange(NE * NE), NE)
    row = np.where(c < 16, 16 * b + c, 288 + 24 * (c - 16) + b)
    inner = np.arange(1, 17)
    low, high = np.zeros(16, int), np.full(16, 17)
    jq = np.concatenate([np.repeat(inner, 16), low, high, inner, inner])
    kq = np.concatenate([np.tile(inner, 16), inner, inner, low, high])
    cols = np.concatenate([np.arange(256), np.tile(np.arange(256, 320), 3)])
    qj, qk, qi = np.zeros((3, 32, 512))
    qe = np.zeros((32, SLOTS))
    qj[jq[cols], np.arange(448)] = 1
    qk[kq[cols], np.arange(448)] = 1
    qi[np.arange(432) % 144 // 8, np.arange(432)] = 1
    qe[1 + np.arange(128) // 8, np.arange(128)] = 1
    qb, qc = np.zeros((2, 32, 1024))
    for t in range(3):
        qb[b, ROWS * t + row] = 1
        qc[c, ROWS * t + row] = 1
    return np.concatenate([qj, qk, qi, qb, qc, qe], axis=1)


def split2(x):
    high = x.astype(BF)
    return high, (x - high.astype(F32)).astype(BF)


def split3(x):
    high = x.astype(BF)
    rest = x - high.astype(F32)
    middle = rest.astype(BF)
    return high, middle, (rest - middle.astype(F32)).astype(BF)


def dot(a, b):
    return jnp.dot(a, b, preferred_element_type=F32)


def widen(small, right):
    return sum(dot(term, right) for term in split3(small))


def pick(condition):
    return jnp.where(condition, 1.0, 0.0).astype(BF)


def aligned(index, step):
    return index if isinstance(index, int) else pl.multiple_of(index, step)


def face_index(face):
    return (slice(None),) * (face // 2) + (14 if face % 2 else 1,)


def list_rows(direction):
    axis, side = direction // 2, direction % 2
    return STARTS[axis] + side * COUNTS[axis], COUNTS[axis]


def find_neighbours(me):
    spot = (lax.rem(me, 4), lax.rem(lax.div(me, 4), 4), lax.div(me, 16))
    tops = (3, 3, 15)
    return [spot[d // 2] > 0 if d % 2 == 0 else spot[d // 2] < tops[d // 2] for d in range(6)]


def greet(me, present):
    barrier = pltpu.get_barrier_semaphore()
    for direction in range(6):

        @pl.when(present[direction])
        def _():
            pl.semaphore_signal(
                barrier, inc=1, device_id=(me + OFFSETS[direction],), device_id_type=pl.DeviceIdType.MESH
            )

    return barrier


def outgoing(me, direction, msgs, arrived, send_sem, recv_sem):
    start, count = list_rows(direction)
    return pltpu.make_async_remote_copy(
        src_ref=msgs.at[pl.ds(start, count)],
        dst_ref=arrived.at[pl.ds(start, count)],
        send_sem=send_sem.at[direction],
        recv_sem=recv_sem.at[direction],
        device_id=(me + OFFSETS[direction],),
        device_id_type=pl.DeviceIdType.MESH,
    )


def send_axis(axis, me, present, parts, send, msgs, arrived, send_sem, recv_sem):
    count = 2 * COUNTS[axis]
    ids = send[axis : axis + 1, :] - 256 * axis
    chosen = pick(lax.broadcasted_iota(jnp.int32, (256, SLOTS), 0) == ids)
    found = dot(parts[axis, 0], chosen) + dot(parts[axis, 1], chosen)
    msgs[STARTS[axis] : STARTS[axis] + count, :] = found.T[:count]


def launch(axis, me, present, msgs, arrived, send_sem, recv_sem):
    for direction in (2 * axis, 2 * axis + 1):

        @pl.when(present[direction])
        def _():
            outgoing(me, direction, msgs, arrived, send_sem, recv_sem).start()


def await_axis(axis, me, present, msgs, arrived, send_sem, recv_sem):
    for direction in (2 * axis, 2 * axis + 1):

        @pl.when(present[direction])
        def _():
            outgoing(me, direction, msgs, arrived, send_sem, recv_sem).wait_send()

        @pl.when(present[direction ^ 1])
        def _():
            outgoing(me, direction, msgs, arrived, send_sem, recv_sem).wait_recv()


def pair(table, axis):
    return jnp.concatenate([table[2 * axis : 2 * axis + 1, :], table[2 * axis + 1 : 2 * axis + 2, :]], axis=1)


def gather_near(axis, parts, found, nbr_src, nbr_idx):
    src = pair(nbr_src, axis)
    idx = pair(nbr_idx, axis)
    here = jnp.where(src == 1, idx - 256 * axis, -1)
    near = pick(lax.broadcasted_iota(jnp.int32, (256, 256), 0) == here)
    found[axis] = dot(parts[axis, 0], near) + dot(parts[axis, 1], near)


def gather_far(axis, arrived, found, out, nbr_src, nbr_idx, orient):
    count = COUNTS[axis]
    src = pair(nbr_src, axis)
    idx = pair(nbr_idx, axis)
    codes = pair(orient, axis)
    there = jnp.where(src == 2 + 2 * axis, idx, jnp.where(src == 3 + 2 * axis, idx + count, -1))
    far = pick(lax.broadcasted_iota(jnp.int32, (2 * count, 256), 0) == there)
    high, low = split2(arrived[STARTS[axis] : STARTS[axis] + 2 * count, :].T)
    found[axis] += dot(high, far) + dot(low, far)
    first = codes % 2 == 1
    second = codes >= 2
    back = 7 - lax.broadcasted_iota(jnp.int32, (8, SLOTS), 0)
    for lanes in (slice(0, SLOTS), slice(SLOTS, 2 * SLOTS)):
        for u in range(16):
            rows = [
                jnp.where(
                    first[:, lanes],
                    found[axis, 16 * (15 - u) + 8 * n : 16 * (15 - u) + 8 * n + 8, lanes],
                    found[axis, 16 * u + 8 * n : 16 * u + 8 * n + 8, lanes],
                )
                for n in (0, 1)
            ]
            for n in (0, 1):
                turned = jnp.take_along_axis(rows[1 - n], back, axis=0)
                out[axis, 16 * u + 8 * n : 16 * u + 8 * n + 8, lanes] = jnp.where(second[:, lanes], turned, rows[n])


def store_terms(value, out, rows, highs, lows):
    high, low = split2(value)
    for start in highs:
        out[rows, start : start + SLOTS] = high
    for start in lows:
        out[rows, start : start + SLOTS] = low


def store_mixed(value, out, rows, start, bound):
    high, low = split2(value)
    lane = lax.broadcasted_iota(jnp.int32, value.shape, 1)
    out[rows, start : start + SLOTS] = jnp.where(lane < bound, high.astype(F32), low.astype(F32)).astype(BF)


def store_tile(value, out, rows, tile, bound):
    start = SLOTS * tile
    if start + SLOTS <= bound:
        store_terms(value, out, rows, (start,), ())
    elif start >= bound:
        store_terms(value, out, rows, (), (start,))
    else:
        store_mixed(value, out, rows, start, bound - start)


def make_operators(s_mats, lam, coeff, right, l1, l2, l4, l5, l5r, d12, d0, factors):
    room = ((0, 14), (0, 14))
    mats = [jnp.pad(s_mats[axis], room) for axis in range(3)]
    turned = [jnp.pad(s_mats[axis].T, room) for axis in range(3)]

    def tail(a, b, join):
        return jnp.concatenate([join(a[0:24], b[16:17]), join(a[0:24], b[17:18])], axis=0)

    first = widen(turned[1], right[:, 0:512])
    second = widen(turned[2], right[:, 512:1024])
    for tile in range(4):
        lanes = slice(SLOTS * tile, SLOTS * tile + SLOTS)
        a, b = first[:, lanes], second[:, lanes]
        blocks = [(slice(16 * n, 16 * n + 16), a[n : n + 1] * b[0:16]) for n in range(NE)]
        blocks.append((slice(288, 336), tail(a, b, jnp.multiply)))
        for rows, value in blocks:
            if tile < 2:
                store_terms(value, l1, rows, (SLOTS * tile, SLOTS * tile + 256), (SLOTS * tile + 512,))
            elif tile == 2:
                store_terms(value, l1, rows, (768,), ())
            else:
                store_terms(value, l1, rows, (), (896,))

    same = (lax.broadcasted_iota(jnp.int32, (8, SLOTS), 0) == (lax.broadcasted_iota(jnp.int32, (8, SLOTS), 1) & 7))
    wide = widen(turned[0], right[:, 3584:3712])
    for n in range(0, NE, 2):
        rows = slice(8 * n, 8 * n + 16)
        value = jnp.concatenate([jnp.where(same, wide[m : m + 1, :SLOTS], 0.0) for m in (n, n + 1)], axis=0)
        store_terms(value, l2, rows, (0, 128), (256,))
    wide = widen(mats[0], right[:, 1024:1536])
    for tile in range(4):
        part = wide[:, SLOTS * tile : SLOTS * tile + SLOTS]
        for n in range(0, NE, 2):
            value = jnp.concatenate([jnp.where(same, part[m : m + 1], 0.0) for m in (n, n + 1)], axis=0)
            store_tile(value, l4, slice(8 * n, 8 * n + 16), tile, 288)

    first = widen(pltpu.roll(mats[1], 31, 0), right[:, 1536:2560])
    second = widen(pltpu.roll(mats[2], 31, 0), right[:, 2560:3584])
    for tile in range(8):
        lanes = slice(SLOTS * tile, SLOTS * tile + SLOTS)
        a, b = first[:, lanes], second[:, lanes]
        values = [a[n : n + 1] * b[0:16] for n in (*range(16), 31, 16)]
        values += [a[0:16] * b[n : n + 1] for n in (31, 16)]
        for n, value in enumerate(values[:16]):
            store_tile(value, l5, slice(16 * n, 16 * n + 16), tile, 2 * ROWS)
        for n, value in enumerate(values[16:] if tile < 3 else ()):
            high, low = split2(value)
            l5r[16 * n : 16 * n + 16, lanes] = high
            l5r[64 + 16 * n : 64 + 16 * n + 16, lanes] = low

    levels = jnp.pad(lam[...], ((0, 5), (0, 110))).T[:32]
    products = [levels[:, axis : axis + 1] * coeff[axis : axis + 1, :] for axis in range(3)]
    for n in range(NE):
        d12[16 * n : 16 * n + 16, :] = products[1][n : n + 1] + products[2][0:16]
        d0[8 * n : 8 * n + 8, :] = jnp.broadcast_to(products[0][n : n + 1], (8, SLOTS))
    sides = [jnp.broadcast_to(turned[0][:, n : n + 1], (32, SLOTS)) for n in (0, 17)]
    for n in range(NE):
        for m in (0, 1):
            factors[m, 8 * n : 8 * n + 8, :] = jnp.broadcast_to(sides[m][n : n + 1], (8, SLOTS))
    d12[288:336, :] = tail(products[1], products[2], jnp.add)


def smooth_kernel(
    field_in, s_mats_in, lam_in, coeff_in, src_in, idx_in, orient_in, send_x_in, send_y_in, send_z_in, right_in,
    solved, back,
    field, s_mats, lam, coeff, nbr_src, nbr_idx, orient, send_x, send_y, send_z, right,
    planes, l1, l2, l4, l5, l5r, d12, d0, factors, send, parts, found, ghosts, mid, coef, edges, shells, u_high, u_low,
    msgs, arrived, load_sem, send_sem, recv_sem,
):
    me = lax.axis_index("dev")
    present = find_neighbours(me)
    for direction in range(6):
        start, count = list_rows(direction)

        @pl.when(jnp.logical_not(present[direction ^ 1]))
        def _():
            for phase in range(2):
                arrived[phase, start : start + count, :] = jnp.zeros((count, 256), F32)

    barrier = greet(me, present)
    loads = [
        pltpu.make_async_copy(source, target, load_sem.at[n])
        for n, (source, target) in enumerate(
            (
                (send_x_in, send_x), (send_y_in, send_y), (send_z_in, send_z),
                *((field_in.at[face_index(face)], planes.at[face]) for face in (2, 3, 4, 5, 0, 1)), (field_in, field),
                (s_mats_in, s_mats), (right_in, right), (lam_in, lam), (coeff_in, coeff),
                (src_in, nbr_src), (idx_in, nbr_idx), (orient_in, orient),
            )
        )
    ]
    for load in loads:
        load.start()
    for load in loads[:9]:
        load.wait()
    send[...] = jnp.full((8, SLOTS), -1, jnp.int32)
    send[0:1, 0:16] = send_x[0:1, :]
    send[0:1, 16:32] = send_x[1:2, :]
    send[1:2, 0:16] = send_y[0:1, :]
    send[1:2, 16:32] = send_y[1:2, :]
    send[2:3, 0:64] = send_z[0:1, :]
    send[2:3, 64:128] = send_z[1:2, :]

    wires = [(me, present, msgs, arrived.at[n], send_sem.at[n], recv_sem.at[n]) for n in range(2)]

    def send_planes(axis, wire):
        send_axis(axis, *wire[:2], parts, send, *wire[2:])

    for axis in (2, 1, 0):
        parts[axis, 0], parts[axis, 1] = split2(
            jnp.concatenate([planes[2 * axis + n].reshape(256, SLOTS) for n in (0, 1)], axis=1)
        )
        send_planes(axis, wires[0])
    pl.semaphore_wait(barrier, sum(jnp.where(flag, 1, 0) for flag in present))
    for axis in (2, 1, 0):
        launch(axis, *wires[0])
    for load in loads[9:]:
        load.wait()
    make_operators(s_mats, lam, coeff, right, l1, l2, l4, l5, l5r, d12, d0, factors)
    for axis in range(3):
        gather_near(axis, parts, found, nbr_src, nbr_idx)

    def forward_inner(t):
        x = jnp.concatenate([field[2 * t + n].reshape(256, SLOTS) for n in (0, 1)], axis=1)
        high, low = split2(x)
        out = dot(l1[:, 0:768], jnp.concatenate([high, low, high], axis=0))
        mid[2 * t + 1] = out[:, :SLOTS]
        mid[2 * t + 2] = out[:, SLOTS:]

    for t in range(8):
        forward_inner(t)

    for start in range(0, ROWS, 16):
        block = mid[1:17, start : start + 16, :]
        y = jnp.concatenate([block[:, 0:8].reshape(SLOTS, SLOTS), block[:, 8:16].reshape(SLOTS, SLOTS)], axis=1)
        high, low = split2(y)
        z = dot(l2[:, 0:384], jnp.concatenate([high, low, high], axis=0))
        coef[:, start : start + 8, :] = z[:, :SLOTS].reshape(NE, 8, SLOTS)
        coef[:, start + 8 : start + 16, :] = z[:, SLOTS:].reshape(NE, 8, SLOTS)

    for axis in (0, 1, 2):
        await_axis(axis, *wires[0])
    for axis in (0, 1, 2):
        gather_far(axis, arrived.at[0], found, ghosts, nbr_src, nbr_idx, orient)

    turned = []
    for axis in (1, 2):
        for half in range(2):
            x = ghosts[axis].reshape(16, 16, 256)[:, 8 * half : 8 * half + 8, :].reshape(SLOTS, 256)
            high, low = split2(x)
            turned.append(dot(l2[:, 0:384], jnp.concatenate([high, low, high], axis=0)))
    high, low = split2(ghosts[0])
    out = dot(l1[:, 0:768], jnp.concatenate([high, low, high], axis=0))
    edges[0] = out[:, :SLOTS]
    edges[1] = out[:, SLOTS:]
    for a in range(0, NE, 2):
        extra = jnp.concatenate(
            [
                jnp.concatenate(
                    [
                        turned[2 * axis + half][8 * n : 8 * n + 8, SLOTS * side : SLOTS * side + SLOTS]
                        for axis in (0, 1)
                        for side in (0, 1)
                        for half in (0, 1)
                    ],
                    axis=0,
                )
                for n in (a, a + 1)
            ],
            axis=1,
        )
        high, low = split2(extra)
        out = dot(l1[:, 768:960], jnp.concatenate([high, low, high], axis=0))
        coef[a] += out[:, :SLOTS]
        coef[a + 1] += out[:, SLOTS:]
    for a in range(0, NE, 2):
        scaled = []
        for n in (a, a + 1):
            rows = slice(8 * n, 8 * n + 8)
            z = coef[n].reshape(42, 8, SLOTS)
            for m in (0, 1):
                z = z + factors[m, rows, :] * edges[m].reshape(42, 8, SLOTS)
            z = (z / (d0[rows, :] + d12[...].reshape(42, 8, SLOTS))).reshape(ROWS, SLOTS)
            coef[n] = z
            scaled.append(z)
        high, low = split2(jnp.concatenate(scaled, axis=1))
        both = dot(l5r[:, 0:ROWS], high)
        out = both[0:64] + both[64:128] + dot(l5r[0:64, 0:ROWS], low)
        shells[a] = out[:, :SLOTS]
        shells[a + 1] = out[:, SLOTS:]
    for axis in (2, 1):
        turned = []
        for half in range(2):
            starts = [32 * (axis - 1) + 16 * side + 8 * half for side in (0, 1)]
            x = jnp.concatenate([shells[:, start : start + 8, :].reshape(144, SLOTS) for start in starts], axis=1)
            high, low = split2(x)
            turned.append(dot(l4[:, 0:432], jnp.concatenate([high, low, high], axis=0)))
        rim = jnp.concatenate([turned[half][8 * i : 8 * i + 8] for i in range(1, 17) for half in range(2)], axis=0)
        parts[axis, 0], parts[axis, 1] = split2(rim)
    for axis in (2, 1):
        send_planes(axis, wires[1])
    for axis in (2, 1):
        launch(axis, *wires[1])
    def middle(g):
        start = pl.multiple_of(16 * g, 16)
        block = coef[:, pl.ds(start, 16), :]
        z = jnp.concatenate([block[:, 0:8].reshape(144, SLOTS), block[:, 8:16].reshape(144, SLOTS)], axis=1)
        high, low = split2(z)
        u = dot(l4[:, 0:432], jnp.concatenate([high, low, high], axis=0))
        high, low = split2(
            jnp.concatenate([u[:, :SLOTS].reshape(NE, 8, SLOTS), u[:, SLOTS:].reshape(NE, 8, SLOTS)], axis=1)
        )
        u_high[:, pl.ds(start, 16), :] = high
        u_low[:, pl.ds(start, 16), :] = low

    @pl.loop(0, 3)
    def _(g):
        for n in range(7):
            middle(7 * g + n)

    def inverse(first, second):
        high = jnp.concatenate([u_high[first], u_high[second]], axis=1)
        low = jnp.concatenate([u_low[first], u_low[second]], axis=1)
        return dot(l5[...], jnp.concatenate([high, low, high, jnp.zeros((16, 256), BF)], axis=0))

    parts[0, 0], parts[0, 1] = split2(inverse(0, 17))
    send_planes(0, wires[1])
    launch(0, *wires[1])
    for t in range(8):
        out = inverse(2 * t + 1, 2 * t + 2)
        solved[512 * t : 512 * t + 256, :] = out[:, :SLOTS]
        solved[512 * t + 256 : 512 * t + 512, :] = out[:, SLOTS:]
    for axis in range(3):
        gather_near(axis, parts, found, nbr_src, nbr_idx)
    for axis in (0, 1, 2):
        await_axis(axis, *wires[1])
    for axis in (0, 1, 2):
        gather_far(axis, arrived.at[1], found, back, nbr_src, nbr_idx, orient)


def finish_kernel(solved, back, out, whole, sems):
    rank = lax.broadcasted_iota(jnp.int32, (16, 16, SLOTS), 1)

    def store(t):
        rows = pl.ds(512 * t, 512)
        return pltpu.make_async_copy(whole.at[rows], out.at[rows], sems.at[t])

    for i in range(16):
        base = 256 * i
        half = slice(16 * i, 16 * i + 16)
        inner = back[2, half, :]
        low = jnp.broadcast_to(inner[:, None, :SLOTS], (16, 16, SLOTS))
        high = jnp.broadcast_to(inner[:, None, SLOTS:], (16, 16, SLOTS))
        value = solved[base : base + 256, :]
        value = value + jnp.where(rank == 1, low, jnp.where(rank == 14, high, 0.0)).reshape(256, SLOTS)
        if i in (1, 14):
            lanes = slice(0, SLOTS) if i == 1 else slice(SLOTS, 2 * SLOTS)
            value = value + back[0, :, lanes]
        whole[base : base + 16, :] = value[0:16]
        whole[base + 16 : base + 32, :] = value[16:32] + back[1, half, :SLOTS]
        whole[base + 32 : base + 224, :] = value[32:224]
        whole[base + 224 : base + 240, :] = value[224:240] + back[1, half, SLOTS:]
        whole[base + 240 : base + 256, :] = value[240:256]
        if i % 2 == 1:
            store(i // 2).start()
    for t in range(8):
        store(t).wait()


def shards(field, s_mats, lam, coeff, nbr_src, nbr_idx, orient, send_x, send_y, send_z):
    right = jnp.asarray(make_tables(), BF)
    inputs = (field, s_mats, lam, coeff, nbr_src, nbr_idx, orient, send_x, send_y, send_z, right)
    solved, back = pl.pallas_call(
        smooth_kernel,
        out_shape=(jax.ShapeDtypeStruct((4096, SLOTS), F32), jax.ShapeDtypeStruct((3, 256, 256), F32)),
        in_specs=[pl.BlockSpec(memory_space=pltpu.HBM)] * 11,
        out_specs=(VMEM, VMEM),
        scratch_shapes=[pltpu.VMEM(value.shape, value.dtype) for value in inputs]
        + [
            pltpu.VMEM((6, 16, 16, SLOTS), F32),
            pltpu.VMEM((ROWS, 1024), BF),
            pltpu.VMEM((144, 384), BF),
            pltpu.VMEM((144, 512), BF),
            pltpu.VMEM((256, 1024), BF),
            pltpu.VMEM((128, 384), BF),
            pltpu.VMEM((ROWS, SLOTS), F32),
            pltpu.VMEM((144, SLOTS), F32),
            pltpu.VMEM((2, 144, SLOTS), F32),
            pltpu.VMEM((8, SLOTS), jnp.int32),
            pltpu.VMEM((3, 2, 256, 256), BF),
            pltpu.VMEM((3, 256, 256), F32),
            pltpu.VMEM((3, 256, 256), F32),
            pltpu.VMEM((NE, ROWS, SLOTS), F32),
            pltpu.VMEM((NE, ROWS, SLOTS), F32),
            pltpu.VMEM((2, ROWS, SLOTS), F32),
            pltpu.VMEM((NE, 64, SLOTS), F32),
            pltpu.VMEM((NE, ROWS, SLOTS), BF),
            pltpu.VMEM((NE, ROWS, SLOTS), BF),
            pltpu.VMEM((192, 256), F32),
            pltpu.VMEM((2, 192, 256), F32),
            pltpu.SemaphoreType.DMA((17,)),
            pltpu.SemaphoreType.DMA((2, 6)),
            pltpu.SemaphoreType.DMA((2, 6)),
        ],
        compiler_params=pltpu.CompilerParams(collective_id=0, has_side_effects=True, vmem_limit_bytes=24 << 20),
        name="smooth",
    )(*(pltpu.with_memory_space_constraint(value, pltpu.HBM) for value in inputs))
    out = pl.pallas_call(
        finish_kernel,
        out_shape=jax.ShapeDtypeStruct((4096, SLOTS), F32),
        in_specs=[VMEM, VMEM],
        out_specs=pl.BlockSpec(memory_space=pltpu.HBM),
        scratch_shapes=[pltpu.VMEM((4096, SLOTS), F32), pltpu.SemaphoreType.DMA((8,))],
        compiler_params=pltpu.CompilerParams(vmem_limit_bytes=8 << 20),
        name="finish",
    )(solved, back)
    return out.reshape(field.shape)


def solution(mesh):
    placed = (
        P(None, None, None, "dev"),
        P(),
        P(),
        P(None, "dev"),
        P(None, "dev"),
        P(None, "dev"),
        P(None, "dev"),
        P(None, "dev"),
        P(None, "dev"),
        P(None, "dev"),
    )
    return jax.shard_map(
        shards, mesh=mesh, in_specs=placed, out_specs=P(None, None, None, "dev"), check_vma=False
    )
```

```python
import functools

import jax
import jax.numpy as jnp
import numpy as np
from jax import lax
from jax.experimental import pallas as pl
from jax.experimental.pallas import tpu as pltpu
from jax.sharding import PartitionSpec as P

NP = 16
NE = 18
SLOTS = 128
ROWS = 336
RIM = 320
COUNTS = (16, 16, 64)
STARTS = (0, 32, 64)
OFFSETS = (-1, 1, -4, 4, -16, 16)
BF = jnp.bfloat16
F32 = jnp.float32
VMEM = pl.BlockSpec(memory_space=pltpu.VMEM)


def make_tables():
    b, c = np.divmod(np.arange(NE * NE), NE)
    row = np.where(c < 16, 16 * b + c, 288 + 24 * (c - 16) + b)
    inner = np.arange(1, 17)
    low, high = np.zeros(16, int), np.full(16, 17)
    jq = np.concatenate([np.repeat(inner, 16), low, high, inner, inner])
    kq = np.concatenate([np.tile(inner, 16), inner, inner, low, high])
    cols = np.concatenate([np.arange(256), np.tile(np.arange(256, 320), 3)])
    qj, qk, qi = np.zeros((3, 32, 512))
    qe = np.zeros((32, SLOTS))
    qj[jq[cols], np.arange(448)] = 1
    qk[kq[cols], np.arange(448)] = 1
    qi[np.arange(432) % 144 // 8, np.arange(432)] = 1
    qe[1 + np.arange(128) // 8, np.arange(128)] = 1
    qb, qc = np.zeros((2, 32, 1024))
    for t in range(3):
        qb[b, ROWS * t + row] = 1
        qc[c, ROWS * t + row] = 1
    return np.concatenate([qj, qk, qi, qb, qc, qe], axis=1)


def split2(x):
    high = x.astype(BF)
    return high, (x - high.astype(F32)).astype(BF)


def split3(x):
    high = x.astype(BF)
    rest = x - high.astype(F32)
    middle = rest.astype(BF)
    return high, middle, (rest - middle.astype(F32)).astype(BF)


def dot(a, b):
    return jnp.dot(a, b, preferred_element_type=F32)


def widen(small, right):
    return sum(dot(term, right) for term in split3(small))


def pick(condition):
    return jnp.where(condition, 1.0, 0.0).astype(BF)


def aligned(index, step):
    return index if isinstance(index, int) else pl.multiple_of(index, step)


def face_index(face):
    return (slice(None),) * (face // 2) + (14 if face % 2 else 1,)


def list_rows(direction):
    axis, side = direction // 2, direction % 2
    return STARTS[axis] + side * COUNTS[axis], COUNTS[axis]


def find_neighbours(me):
    spot = (lax.rem(me, 4), lax.rem(lax.div(me, 4), 4), lax.div(me, 16))
    tops = (3, 3, 15)
    return [spot[d // 2] > 0 if d % 2 == 0 else spot[d // 2] < tops[d // 2] for d in range(6)]


def greet(me, present):
    barrier = pltpu.get_barrier_semaphore()
    for direction in range(6):

        @pl.when(present[direction])
        def _():
            pl.semaphore_signal(
                barrier, inc=1, device_id=(me + OFFSETS[direction],), device_id_type=pl.DeviceIdType.MESH
            )

    return barrier


def outgoing(me, direction, msgs, arrived, send_sem, recv_sem):
    start, count = list_rows(direction)
    return pltpu.make_async_remote_copy(
        src_ref=msgs.at[pl.ds(start, count)],
        dst_ref=arrived.at[pl.ds(start, count)],
        send_sem=send_sem.at[direction],
        recv_sem=recv_sem.at[direction],
        device_id=(me + OFFSETS[direction],),
        device_id_type=pl.DeviceIdType.MESH,
    )


def send_axis(axis, me, present, parts, send, msgs, arrived, send_sem, recv_sem):
    count = 2 * COUNTS[axis]
    ids = send[axis : axis + 1, :] - 256 * axis
    chosen = pick(lax.broadcasted_iota(jnp.int32, (256, SLOTS), 0) == ids)
    found = dot(parts[axis, 0], chosen) + dot(parts[axis, 1], chosen)
    msgs[STARTS[axis] : STARTS[axis] + count, :] = found.T[:count]


def launch(axis, me, present, msgs, arrived, send_sem, recv_sem):
    for direction in (2 * axis, 2 * axis + 1):

        @pl.when(present[direction])
        def _():
            outgoing(me, direction, msgs, arrived, send_sem, recv_sem).start()


def await_axis(axis, me, present, msgs, arrived, send_sem, recv_sem):
    for direction in (2 * axis, 2 * axis + 1):

        @pl.when(present[direction])
        def _():
            outgoing(me, direction, msgs, arrived, send_sem, recv_sem).wait_send()

        @pl.when(present[direction ^ 1])
        def _():
            outgoing(me, direction, msgs, arrived, send_sem, recv_sem).wait_recv()


def pair(table, axis):
    return jnp.concatenate([table[2 * axis : 2 * axis + 1, :], table[2 * axis + 1 : 2 * axis + 2, :]], axis=1)


def gather_near(axis, parts, found, nbr_src, nbr_idx):
    src = pair(nbr_src, axis)
    idx = pair(nbr_idx, axis)
    here = jnp.where(src == 1, idx - 256 * axis, -1)
    near = pick(lax.broadcasted_iota(jnp.int32, (256, 256), 0) == here)
    found[axis] = dot(parts[axis, 0], near) + dot(parts[axis, 1], near)


def gather_far(axis, arrived, found, out, nbr_src, nbr_idx, orient):
    count = COUNTS[axis]
    src = pair(nbr_src, axis)
    idx = pair(nbr_idx, axis)
    codes = pair(orient, axis)
    there = jnp.where(src == 2 + 2 * axis, idx, jnp.where(src == 3 + 2 * axis, idx + count, -1))
    far = pick(lax.broadcasted_iota(jnp.int32, (2 * count, 256), 0) == there)
    high, low = split2(arrived[STARTS[axis] : STARTS[axis] + 2 * count, :].T)
    found[axis] += dot(high, far) + dot(low, far)
    first = codes % 2 == 1
    second = codes >= 2
    back = 7 - lax.broadcasted_iota(jnp.int32, (8, SLOTS), 0)
    for lanes in (slice(0, SLOTS), slice(SLOTS, 2 * SLOTS)):
        for u in range(16):
            rows = [
                jnp.where(
                    first[:, lanes],
                    found[axis, 16 * (15 - u) + 8 * n : 16 * (15 - u) + 8 * n + 8, lanes],
                    found[axis, 16 * u + 8 * n : 16 * u + 8 * n + 8, lanes],
                )
                for n in (0, 1)
            ]
            for n in (0, 1):
                turned = jnp.take_along_axis(rows[1 - n], back, axis=0)
                out[axis, 16 * u + 8 * n : 16 * u + 8 * n + 8, lanes] = jnp.where(second[:, lanes], turned, rows[n])


def store_terms(value, out, rows, highs, lows):
    high, low = split2(value)
    for start in highs:
        out[rows, start : start + SLOTS] = high
    for start in lows:
        out[rows, start : start + SLOTS] = low


def store_mixed(value, out, rows, start, bound):
    high, low = split2(value)
    lane = lax.broadcasted_iota(jnp.int32, value.shape, 1)
    out[rows, start : start + SLOTS] = jnp.where(lane < bound, high.astype(F32), low.astype(F32)).astype(BF)


def store_tile(value, out, rows, tile, bound):
    start = SLOTS * tile
    if start + SLOTS <= bound:
        store_terms(value, out, rows, (start,), ())
    elif start >= bound:
        store_terms(value, out, rows, (), (start,))
    else:
        store_mixed(value, out, rows, start, bound - start)


def make_operators(s_mats, lam, coeff, right, l1, l2, l4, l5, l5r, d12, d0, factors):
    room = ((0, 14), (0, 14))
    mats = [jnp.pad(s_mats[axis], room) for axis in range(3)]
    turned = [jnp.pad(s_mats[axis].T, room) for axis in range(3)]

    def tail(a, b, join):
        return jnp.concatenate([join(a[0:24], b[16:17]), join(a[0:24], b[17:18])], axis=0)

    first = widen(turned[1], right[:, 0:512])
    second = widen(turned[2], right[:, 512:1024])
    for tile in range(4):
        lanes = slice(SLOTS * tile, SLOTS * tile + SLOTS)
        a, b = first[:, lanes], second[:, lanes]
        blocks = [(slice(16 * n, 16 * n + 16), a[n : n + 1] * b[0:16]) for n in range(NE)]
        blocks.append((slice(288, 336), tail(a, b, jnp.multiply)))
        for rows, value in blocks:
            if tile < 2:
                store_terms(value, l1, rows, (SLOTS * tile, SLOTS * tile + 256), (SLOTS * tile + 512,))
            elif tile == 2:
                store_terms(value, l1, rows, (768,), ())
            else:
                store_terms(value, l1, rows, (), (896,))

    same = (lax.broadcasted_iota(jnp.int32, (8, SLOTS), 0) == (lax.broadcasted_iota(jnp.int32, (8, SLOTS), 1) & 7))
    wide = widen(turned[0], right[:, 3584:3712])
    for n in range(0, NE, 2):
        rows = slice(8 * n, 8 * n + 16)
        value = jnp.concatenate([jnp.where(same, wide[m : m + 1, :SLOTS], 0.0) for m in (n, n + 1)], axis=0)
        store_terms(value, l2, rows, (0, 128), (256,))
    wide = widen(mats[0], right[:, 1024:1536])
    for tile in range(4):
        part = wide[:, SLOTS * tile : SLOTS * tile + SLOTS]
        for n in range(0, NE, 2):
            value = jnp.concatenate([jnp.where(same, part[m : m + 1], 0.0) for m in (n, n + 1)], axis=0)
            store_tile(value, l4, slice(8 * n, 8 * n + 16), tile, 288)

    first = widen(pltpu.roll(mats[1], 31, 0), right[:, 1536:2560])
    second = widen(pltpu.roll(mats[2], 31, 0), right[:, 2560:3584])
    for tile in range(8):
        lanes = slice(SLOTS * tile, SLOTS * tile + SLOTS)
        a, b = first[:, lanes], second[:, lanes]
        values = [a[n : n + 1] * b[0:16] for n in (*range(16), 31, 16)]
        values += [a[0:16] * b[n : n + 1] for n in (31, 16)]
        for n, value in enumerate(values[:16]):
            store_tile(value, l5, slice(16 * n, 16 * n + 16), tile, 2 * ROWS)
        for n, value in enumerate(values[16:] if tile < 3 else ()):
            high, low = split2(value)
            l5r[16 * n : 16 * n + 16, lanes] = high
            l5r[64 + 16 * n : 64 + 16 * n + 16, lanes] = low

    levels = jnp.pad(lam[...], ((0, 5), (0, 110))).T[:32]
    products = [levels[:, axis : axis + 1] * coeff[axis : axis + 1, :] for axis in range(3)]
    for n in range(NE):
        d12[16 * n : 16 * n + 16, :] = products[1][n : n + 1] + products[2][0:16]
        d0[8 * n : 8 * n + 8, :] = jnp.broadcast_to(products[0][n : n + 1], (8, SLOTS))
    sides = [jnp.broadcast_to(turned[0][:, n : n + 1], (32, SLOTS)) for n in (0, 17)]
    for n in range(NE):
        for m in (0, 1):
            factors[m, 8 * n : 8 * n + 8, :] = jnp.broadcast_to(sides[m][n : n + 1], (8, SLOTS))
    d12[288:336, :] = tail(products[1], products[2], jnp.add)


def smooth_kernel(
    field_in, s_mats_in, lam_in, coeff_in, src_in, idx_in, orient_in, send_x_in, send_y_in, send_z_in, right_in,
    solved, back,
    field, s_mats, lam, coeff, nbr_src, nbr_idx, orient, send_x, send_y, send_z, right,
    planes, l1, l2, l4, l5, l5r, d12, d0, factors, send, parts, found, ghosts, mid, coef, edges, shells, u_high, u_low,
    msgs, arrived, load_sem, send_sem, recv_sem,
):
    me = lax.axis_index("dev")
    present = find_neighbours(me)
    for direction in range(6):
        start, count = list_rows(direction)

        @pl.when(jnp.logical_not(present[direction ^ 1]))
        def _():
            for phase in range(2):
                arrived[phase, start : start + count, :] = jnp.zeros((count, 256), F32)

    barrier = greet(me, present)
    loads = [
        pltpu.make_async_copy(source, target, load_sem.at[n])
        for n, (source, target) in enumerate(
            (
                (send_z_in, send_z), (send_y_in, send_y),
                *((field_in.at[face_index(face)], planes.at[face]) for face in (4, 5, 2, 3)),
                (send_x_in, send_x),
                *((field_in.at[face_index(face)], planes.at[face]) for face in (0, 1)),
                (s_mats_in, s_mats), (right_in, right), (lam_in, lam), (coeff_in, coeff),
                (field_in, field), (src_in, nbr_src), (idx_in, nbr_idx), (orient_in, orient),
            )
        )
    ]
    for load in loads[:9]:
        load.start()
    for load in loads[:6]:
        load.wait()
    for load in loads[9:]:
        load.start()
    send[...] = jnp.full((8, SLOTS), -1, jnp.int32)
    send[1:2, 0:16] = send_y[0:1, :]
    send[1:2, 16:32] = send_y[1:2, :]
    send[2:3, 0:64] = send_z[0:1, :]
    send[2:3, 64:128] = send_z[1:2, :]

    wires = [(me, present, msgs, arrived.at[n], send_sem.at[n], recv_sem.at[n]) for n in range(2)]

    def send_planes(axis, wire):
        send_axis(axis, *wire[:2], parts, send, *wire[2:])

    def prepare(axis):
        parts[axis, 0], parts[axis, 1] = split2(
            jnp.concatenate([planes[2 * axis + n].reshape(256, SLOTS) for n in (0, 1)], axis=1)
        )
        send_planes(axis, wires[0])

    for axis in (2, 1):
        prepare(axis)
    pl.semaphore_wait(barrier, sum(jnp.where(flag, 1, 0) for flag in present))
    for axis in (2, 1):
        launch(axis, *wires[0])
    for load in loads[6:9]:
        load.wait()
    send[0:1, 0:16] = send_x[0:1, :]
    send[0:1, 16:32] = send_x[1:2, :]
    prepare(0)
    launch(0, *wires[0])
    for load in loads[9:]:
        load.wait()
    make_operators(s_mats, lam, coeff, right, l1, l2, l4, l5, l5r, d12, d0, factors)
    for axis in range(3):
        gather_near(axis, parts, found, nbr_src, nbr_idx)

    def forward_inner(t):
        x = jnp.concatenate([field[2 * t + n].reshape(256, SLOTS) for n in (0, 1)], axis=1)
        high, low = split2(x)
        out = dot(l1[:, 0:768], jnp.concatenate([high, low, high], axis=0))
        mid[2 * t + 1] = out[:, :SLOTS]
        mid[2 * t + 2] = out[:, SLOTS:]

    for t in range(8):
        forward_inner(t)

    for start in range(0, ROWS, 16):
        block = mid[1:17, start : start + 16, :]
        y = jnp.concatenate([block[:, 0:8].reshape(SLOTS, SLOTS), block[:, 8:16].reshape(SLOTS, SLOTS)], axis=1)
        high, low = split2(y)
        z = dot(l2[:, 0:384], jnp.concatenate([high, low, high], axis=0))
        coef[:, start : start + 8, :] = z[:, :SLOTS].reshape(NE, 8, SLOTS)
        coef[:, start + 8 : start + 16, :] = z[:, SLOTS:].reshape(NE, 8, SLOTS)

    for axis in (0, 1, 2):
        await_axis(axis, *wires[0])
    for axis in (0, 1, 2):
        gather_far(axis, arrived.at[0], found, ghosts, nbr_src, nbr_idx, orient)

    turned = []
    for axis in (1, 2):
        for half in range(2):
            x = ghosts[axis].reshape(16, 16, 256)[:, 8 * half : 8 * half + 8, :].reshape(SLOTS, 256)
            high, low = split2(x)
            turned.append(dot(l2[:, 0:384], jnp.concatenate([high, low, high], axis=0)))
    high, low = split2(ghosts[0])
    out = dot(l1[:, 0:768], jnp.concatenate([high, low, high], axis=0))
    edges[0] = out[:, :SLOTS]
    edges[1] = out[:, SLOTS:]
    for a in range(0, NE, 2):
        extra = jnp.concatenate(
            [
                jnp.concatenate(
                    [
                        turned[2 * axis + half][8 * n : 8 * n + 8, SLOTS * side : SLOTS * side + SLOTS]
                        for axis in (0, 1)
                        for side in (0, 1)
                        for half in (0, 1)
                    ],
                    axis=0,
                )
                for n in (a, a + 1)
            ],
            axis=1,
        )
        high, low = split2(extra)
        out = dot(l1[:, 768:960], jnp.concatenate([high, low, high], axis=0))
        coef[a] += out[:, :SLOTS]
        coef[a + 1] += out[:, SLOTS:]
    for a in range(0, NE, 2):
        scaled = []
        for n in (a, a + 1):
            rows = slice(8 * n, 8 * n + 8)
            z = coef[n].reshape(42, 8, SLOTS)
            for m in (0, 1):
                z = z + factors[m, rows, :] * edges[m].reshape(42, 8, SLOTS)
            z = (z / (d0[rows, :] + d12[...].reshape(42, 8, SLOTS))).reshape(ROWS, SLOTS)
            coef[n] = z
            scaled.append(z)
        high, low = split2(jnp.concatenate(scaled, axis=1))
        both = dot(l5r[:, 0:ROWS], high)
        out = both[0:64] + both[64:128] + dot(l5r[0:64, 0:ROWS], low)
        shells[a] = out[:, :SLOTS]
        shells[a + 1] = out[:, SLOTS:]
    for axis in (2, 1):
        turned = []
        for half in range(2):
            starts = [32 * (axis - 1) + 16 * side + 8 * half for side in (0, 1)]
            x = jnp.concatenate([shells[:, start : start + 8, :].reshape(144, SLOTS) for start in starts], axis=1)
            high, low = split2(x)
            turned.append(dot(l4[:, 0:432], jnp.concatenate([high, low, high], axis=0)))
        rim = jnp.concatenate([turned[half][8 * i : 8 * i + 8] for i in range(1, 17) for half in range(2)], axis=0)
        parts[axis, 0], parts[axis, 1] = split2(rim)
    for axis in (2, 1):
        send_planes(axis, wires[1])
    for axis in (2, 1):
        launch(axis, *wires[1])
    def middle(g):
        start = pl.multiple_of(16 * g, 16)
        block = coef[:, pl.ds(start, 16), :]
        z = jnp.concatenate([block[:, 0:8].reshape(144, SLOTS), block[:, 8:16].reshape(144, SLOTS)], axis=1)
        high, low = split2(z)
        u = dot(l4[:, 0:432], jnp.concatenate([high, low, high], axis=0))
        high, low = split2(
            jnp.concatenate([u[:, :SLOTS].reshape(NE, 8, SLOTS), u[:, SLOTS:].reshape(NE, 8, SLOTS)], axis=1)
        )
        u_high[:, pl.ds(start, 16), :] = high
        u_low[:, pl.ds(start, 16), :] = low

    @pl.loop(0, 3)
    def _(g):
        for n in range(7):
            middle(7 * g + n)

    def inverse(first, second):
        high = jnp.concatenate([u_high[first], u_high[second]], axis=1)
        low = jnp.concatenate([u_low[first], u_low[second]], axis=1)
        return dot(l5[...], jnp.concatenate([high, low, high, jnp.zeros((16, 256), BF)], axis=0))

    parts[0, 0], parts[0, 1] = split2(inverse(0, 17))
    send_planes(0, wires[1])
    launch(0, *wires[1])
    for t in range(8):
        out = inverse(2 * t + 1, 2 * t + 2)
        solved[512 * t : 512 * t + 256, :] = out[:, :SLOTS]
        solved[512 * t + 256 : 512 * t + 512, :] = out[:, SLOTS:]
    for axis in range(3):
        gather_near(axis, parts, found, nbr_src, nbr_idx)
    for axis in (0, 1, 2):
        await_axis(axis, *wires[1])
    for axis in (0, 1, 2):
        gather_far(axis, arrived.at[1], found, back, nbr_src, nbr_idx, orient)


def finish_kernel(solved, back, out, whole, sems):
    rank = lax.broadcasted_iota(jnp.int32, (16, 16, SLOTS), 1)

    def store(t):
        rows = pl.ds(512 * t, 512)
        return pltpu.make_async_copy(whole.at[rows], out.at[rows], sems.at[t])

    for i in range(16):
        base = 256 * i
        half = slice(16 * i, 16 * i + 16)
        inner = back[2, half, :]
        low = jnp.broadcast_to(inner[:, None, :SLOTS], (16, 16, SLOTS))
        high = jnp.broadcast_to(inner[:, None, SLOTS:], (16, 16, SLOTS))
        value = solved[base : base + 256, :]
        value = value + jnp.where(rank == 1, low, jnp.where(rank == 14, high, 0.0)).reshape(256, SLOTS)
        if i in (1, 14):
            lanes = slice(0, SLOTS) if i == 1 else slice(SLOTS, 2 * SLOTS)
            value = value + back[0, :, lanes]
        whole[base : base + 16, :] = value[0:16]
        whole[base + 16 : base + 32, :] = value[16:32] + back[1, half, :SLOTS]
        whole[base + 32 : base + 224, :] = value[32:224]
        whole[base + 224 : base + 240, :] = value[224:240] + back[1, half, SLOTS:]
        whole[base + 240 : base + 256, :] = value[240:256]
        if i % 2 == 1:
            store(i // 2).start()
    for t in range(8):
        store(t).wait()


def shards(field, s_mats, lam, coeff, nbr_src, nbr_idx, orient, send_x, send_y, send_z):
    right = jnp.asarray(make_tables(), BF)
    inputs = (field, s_mats, lam, coeff, nbr_src, nbr_idx, orient, send_x, send_y, send_z, right)
    solved, back = pl.pallas_call(
        smooth_kernel,
        out_shape=(jax.ShapeDtypeStruct((4096, SLOTS), F32), jax.ShapeDtypeStruct((3, 256, 256), F32)),
        in_specs=[pl.BlockSpec(memory_space=pltpu.HBM)] * 11,
        out_specs=(VMEM, VMEM),
        scratch_shapes=[pltpu.VMEM(value.shape, value.dtype) for value in inputs]
        + [
            pltpu.VMEM((6, 16, 16, SLOTS), F32),
            pltpu.VMEM((ROWS, 1024), BF),
            pltpu.VMEM((144, 384), BF),
            pltpu.VMEM((144, 512), BF),
            pltpu.VMEM((256, 1024), BF),
            pltpu.VMEM((128, 384), BF),
            pltpu.VMEM((ROWS, SLOTS), F32),
            pltpu.VMEM((144, SLOTS), F32),
            pltpu.VMEM((2, 144, SLOTS), F32),
            pltpu.VMEM((8, SLOTS), jnp.int32),
            pltpu.VMEM((3, 2, 256, 256), BF),
            pltpu.VMEM((3, 256, 256), F32),
            pltpu.VMEM((3, 256, 256), F32),
            pltpu.VMEM((NE, ROWS, SLOTS), F32),
            pltpu.VMEM((NE, ROWS, SLOTS), F32),
            pltpu.VMEM((2, ROWS, SLOTS), F32),
            pltpu.VMEM((NE, 64, SLOTS), F32),
            pltpu.VMEM((NE, ROWS, SLOTS), BF),
            pltpu.VMEM((NE, ROWS, SLOTS), BF),
            pltpu.VMEM((192, 256), F32),
            pltpu.VMEM((2, 192, 256), F32),
            pltpu.SemaphoreType.DMA((17,)),
            pltpu.SemaphoreType.DMA((2, 6)),
            pltpu.SemaphoreType.DMA((2, 6)),
        ],
        compiler_params=pltpu.CompilerParams(collective_id=0, has_side_effects=True, vmem_limit_bytes=24 << 20),
        name="smooth",
    )(*(pltpu.with_memory_space_constraint(value, pltpu.HBM) for value in inputs))
    out = pl.pallas_call(
        finish_kernel,
        out_shape=jax.ShapeDtypeStruct((4096, SLOTS), F32),
        in_specs=[VMEM, VMEM],
        out_specs=pl.BlockSpec(memory_space=pltpu.HBM),
        scratch_shapes=[pltpu.VMEM((4096, SLOTS), F32), pltpu.SemaphoreType.DMA((8,))],
        compiler_params=pltpu.CompilerParams(vmem_limit_bytes=8 << 20),
        name="finish",
    )(solved, back)
    return out.reshape(field.shape)


def solution(mesh):
    placed = (
        P(None, None, None, "dev"),
        P(),
        P(),
        P(None, "dev"),
        P(None, "dev"),
        P(None, "dev"),
        P(None, "dev"),
        P(None, "dev"),
        P(None, "dev"),
        P(None, "dev"),
    )
    return jax.shard_map(
        shards, mesh=mesh, in_specs=placed, out_specs=P(None, None, None, "dev"), check_vma=False
    )
```
